32 devices in a mesh: rows: 4 (over y, x), cols: 8 (over z, core).
Axes of the slice: x: 2, y: 2, z: 4, core: 2. Of those that a mesh axis runs over, the one named last changes fastest.
Arguments:
- object_field: float32 [2, 1024, 2048], P(None, 'rows', 'cols'), may hold values from -6 to 6
- probe: float32 [2, 256, 256], replicated, may hold values from -6 to 6
- positions: int32 [4, 8, 6, 2], P('rows', 'cols'), may hold values from 0 to 256
- counts: int32 [4, 8], P('rows', 'cols'), may hold values from 2 to 6
- intensity: int32 [4, 8, 6, 256, 256], P('rows', 'cols'), may hold values from 0 to 4000
Outputs:
- updated_field: float32 [2, 1024, 2048], P(None, 'rows', 'cols')
The draws below stay inside these ranges and needn't reach their ends.
Inputs may be any that keep to these rules, and one draw needn't show every extreme that they name: Only the first counts[a, b] entries of tile (a, b) in positions and intensity are used.
All inputs are finite; a program needn't handle non-finite values.
Results may differ from the reference program's by a relative error of at most 0.00029.
Values sent between devices are 32-bit elements; how exact they have to be, the bound alone decides.
A program may use at most 64 MiB of HBM per device.

```python
import jax
import jax.numpy as jnp
from jax import lax

TILE = 256
MARGIN = 128
PATCH = 256
SLOTS = 6
ITERS = 2
IMG_R = 1024
IMG_C = 2048
N_ROWS = 4
N_COLS = 8


def with_ends(values, rng, low, high):
    dims = values.shape
    place = [jax.random.randint(jax.random.fold_in(rng, axis), (), 0, dims[axis]) for axis in range(len(dims))]
    values = values.at[tuple(place)].set(low)
    longest = dims.index(max(dims))
    place[longest] = (place[longest] + 1) % dims[longest]
    return values.at[tuple(place)].set(high)


def levels(rng, shape, pieces, least, high):
    def one(dim, parts):
        steps = jax.random.uniform(jax.random.fold_in(jax.random.fold_in(rng, 6), dim), (parts,), jnp.float32, least / len(pieces), high / len(pieces))
        return jnp.repeat(jnp.exp(steps), shape[dim] // parts).reshape((-1,) + (1,) * (len(shape) - dim - 1))

    loudness = one(*pieces[0])
    for cut in pieces[1:]:
        loudness = loudness * one(*cut)
    return loudness


def scatter_about(rng, extent, width, bound, split=(), kind=jnp.bfloat16):
    level = levels(rng, extent, split, -0.22, 0.18) if split else 1.0
    result = jax.random.normal(rng, extent, jnp.float32) * width * level
    return jnp.minimum(jnp.maximum(result, -bound), bound).astype(kind)


def setup_inputs(seed: int = 0) -> dict:
    keys = jax.random.split(jax.random.key(seed), 6)
    object_field = scatter_about(keys[0], (2, IMG_R, IMG_C), 1.0, 6.0, ((1, 4), (2, 8)), jnp.float32)
    probe = scatter_about(keys[1], (2, PATCH, PATCH), 1.0, 6.0, (), jnp.float32)
    positions = with_ends(jax.random.randint(keys[2], (N_ROWS, N_COLS, SLOTS, 2), 0, TILE + 2 * MARGIN - PATCH + 1), jax.random.fold_in(keys[2], 1), 0, TILE + 2 * MARGIN - PATCH).astype(jnp.int32)
    counts = with_ends(jax.random.randint(keys[3], (N_ROWS, N_COLS), 2, SLOTS + 1), jax.random.fold_in(keys[3], 1), 2, SLOTS).astype(jnp.int32)
    intensity = with_ends(jax.random.randint(keys[4], (N_ROWS, N_COLS, SLOTS, PATCH, PATCH), 0, 4001), jax.random.fold_in(keys[4], 1), 0, 4000).astype(jnp.int32)
    return {"object_field": object_field, "probe": probe, "positions": positions, "counts": counts, "intensity": intensity}


step_rate = 0.02
photon_unit = 0.001


def reference(object_field, probe, positions, counts, intensity):
    field = object_field
    probe_c = lax.complex(probe[0], probe[1])
    measured = intensity.astype(field.dtype) * photon_unit
    total = N_ROWS * N_COLS * SLOTS
    for step in range(ITERS):
        padded = jnp.pad(field, ((0, 0), (MARGIN, MARGIN), (MARGIN, MARGIN)))

        def one(item, grad):
            tile = item // SLOTS
            slot = item % SLOTS
            trow = tile // N_COLS
            tcol = tile % N_COLS
            srow = (positions[trow, tcol, slot, 0] + trow * TILE).astype(jnp.int32)
            scol = (positions[trow, tcol, slot, 1] + tcol * TILE).astype(jnp.int32)
            zero = jnp.zeros((), jnp.int32)
            patch = lax.dynamic_slice(padded, (zero, srow, scol), (2, PATCH, PATCH))
            exit_wave = probe_c * lax.complex(patch[0], patch[1])
            spectrum = jnp.fft.fft2(exit_wave, norm="ortho")
            misfit = jnp.real(spectrum) ** 2 + jnp.imag(spectrum) ** 2 - measured[trow, tcol, slot]
            back = jnp.fft.ifft2(misfit * spectrum, norm="ortho")
            term = jnp.conj(probe_c) * back
            live = (slot < counts[trow, tcol]).astype(field.dtype)
            stacked = jnp.stack([jnp.real(term), jnp.imag(term)]) * live
            old = lax.dynamic_slice(grad, (zero, srow, scol), (2, PATCH, PATCH))
            return lax.dynamic_update_slice(grad, old + stacked, (zero, srow, scol))

        grad = lax.fori_loop(0, total, one, jnp.zeros_like(padded))
        field = field - step_rate * grad[:, MARGIN:MARGIN + IMG_R, MARGIN:MARGIN + IMG_C]
    return field
```

```python
import functools

import jax
import jax.numpy as jnp
import numpy as np
from jax import lax
from jax.experimental import pallas as pl
from jax.experimental.pallas import tpu as pltpu
from jax.sharding import PartitionSpec as P

MARGIN = 128
ITERS = 2
LANES = 128
ROWS = 8


step_rate = 0.02
photon_unit = 0.001


def tables(length):
    half = length // 2
    k = np.arange(half)[:, None]
    n = np.arange(half)[None, :]
    found = []
    for odd in (0, 1):
        angle = ((2 * k + odd) * n % length) * (2.0 * np.pi / length)
        c = np.cos(angle) / np.sqrt(length)
        s = np.sin(angle) / np.sqrt(length)
        full = np.block([[c, s], [-s, c]])
        found += [full, full.T]
    full = np.stack(found).astype(np.float32)
    high = full.astype(jnp.bfloat16)
    low = (full - high.astype(np.float32)).astype(jnp.bfloat16)
    return np.stack([high, low])


def ordering(length):
    half = length // 2
    index = np.arange(half)
    table = np.zeros((length, length), np.float32)
    table[2 * index, index] = 1
    table[2 * index + 1, half + index] = 1
    return np.stack([table, table.T]).astype(jnp.bfloat16)


def dot(left, right):
    return lax.dot_general(left, right, (((1,), (0,)), ((), ())), preferred_element_type=jnp.float32)


def parted(value):
    high = value.astype(jnp.bfloat16)
    return high, (value - high.astype(jnp.float32)).astype(jnp.bfloat16)


def from_left(table, which, value):
    high, low = parted(value)
    return dot(table[0, which], high) + dot(table[1, which], high) + dot(table[0, which], low)


def from_right(table, which, value):
    high, low = parted(value)
    return dot(high, table[0, which]) + dot(high, table[1, which]) + dot(low, table[0, which])


def order_kernel(counts_ref, order_ref, intensity_ref, out_ref):
    @pl.loop(0, counts_ref[0, 0])
    def _(slot):
        given = intensity_ref[slot]

        def placed(value):
            value = value.astype(jnp.float32).astype(jnp.bfloat16)
            return dot(dot(order_ref[1], value).astype(jnp.bfloat16), order_ref[0])

        out_ref[slot] = (placed(given >> 4) * 16.0 + placed(given & 15)) * photon_unit


def moved_up(value, shift):
    rows, columns = value.shape
    groups = value.reshape(rows // ROWS, ROWS, columns)
    turned = pltpu.roll(groups, (ROWS - shift) % ROWS, 1)
    within = lax.broadcasted_iota(jnp.int32, (1, ROWS, columns), 1) < ROWS - shift
    return jnp.where(within, turned[:-1], turned[1:]).reshape(rows - ROWS, columns)


def moved_down(value, shift):
    rows, columns = value.shape
    groups = value.reshape(rows // ROWS, ROWS, columns)
    turned = pltpu.roll(groups, shift % ROWS, 1)
    none = jnp.zeros((1, ROWS, columns), value.dtype)
    within = lax.broadcasted_iota(jnp.int32, (1, ROWS, columns), 1) >= shift
    lower = jnp.concatenate([turned, none], axis=0)
    upper = jnp.concatenate([none, turned], axis=0)
    return jnp.where(within, lower, upper).reshape(rows + ROWS, columns)


def moved_left(value, shift):
    rows, columns = value.shape
    parts = [pltpu.roll(value[:, c : c + LANES], (LANES - shift) % LANES, 1) for c in range(0, columns, LANES)]
    within = lax.broadcasted_iota(jnp.int32, (rows, LANES), 1) < LANES - shift
    return jnp.concatenate([jnp.where(within, a, b) for a, b in zip(parts[:-1], parts[1:])], axis=1)


def moved_right(value, shift):
    rows, columns = value.shape
    parts = [pltpu.roll(value[:, c : c + LANES], shift % LANES, 1) for c in range(0, columns, LANES)]
    within = lax.broadcasted_iota(jnp.int32, (rows, LANES), 1) >= shift
    none = jnp.zeros((rows, LANES), value.dtype)
    return jnp.concatenate([jnp.where(within, a, b) for a, b in zip(parts + [none], [none] + parts)], axis=1)


def slots_kernel(positions_ref, counts_ref, padded_ref, probe_ref, measured_ref, table_ref, grad_ref):
    size = probe_ref.shape[1]
    half = size // 2
    wide = size + LANES
    last = padded_ref.shape[1] - size - ROWS
    grad_ref[...] = jnp.zeros_like(grad_ref)

    @pl.loop(0, counts_ref[0, 0])
    def _(slot):
        row = positions_ref[0, 0, slot, 0]
        column = positions_ref[0, 0, slot, 1]
        start = pl.multiple_of(jnp.where(column >= LANES, LANES, 0), LANES)
        shift = column - start
        first = pl.multiple_of(jnp.minimum(row // ROWS * ROWS, last), ROWS)
        drop = row - first
        there = (pl.ds(first, size + ROWS), pl.ds(start, wide))
        patch_r = moved_left(moved_up(padded_ref[(0, *there)], drop), shift)
        patch_i = moved_left(moved_up(padded_ref[(1, *there)], drop), shift)
        probe_r = probe_ref[0]
        probe_i = probe_ref[1]
        exit_r = probe_r * patch_r - probe_i * patch_i
        exit_i = probe_r * patch_i + probe_i * patch_r
        upper = jnp.concatenate([exit_r[:half], exit_i[:half]], axis=0)
        lower = jnp.concatenate([exit_r[half:], exit_i[half:]], axis=0)
        even = from_left(table_ref, 0, upper + lower)
        odd = from_left(table_ref, 2, upper - lower)
        half_r = jnp.concatenate([even[:half], odd[:half]], axis=0)
        half_i = jnp.concatenate([even[half:], odd[half:]], axis=0)
        left = jnp.concatenate([half_r[:, :half], half_i[:, :half]], axis=1)
        right = jnp.concatenate([half_r[:, half:], half_i[:, half:]], axis=1)
        backs = []
        for odd, value in ((0, left + right), (1, left - right)):
            spec = from_right(table_ref, 2 * odd + 1, value)
            spec_r, spec_i = spec[:, :half], spec[:, half:]
            misfit = spec_r * spec_r + spec_i * spec_i - measured_ref[slot, :, odd * half : (odd + 1) * half]
            scaled = jnp.concatenate([misfit * spec_r, misfit * spec_i], axis=1)
            backs.append(from_right(table_ref, 2 * odd, scaled))
        left = backs[0] + backs[1]
        right = backs[0] - backs[1]
        half_r = jnp.concatenate([left[:, :half], right[:, :half]], axis=1)
        half_i = jnp.concatenate([left[:, half:], right[:, half:]], axis=1)
        even = from_left(table_ref, 1, jnp.concatenate([half_r[:half], half_i[:half]], axis=0))
        odd = from_left(table_ref, 3, jnp.concatenate([half_r[half:], half_i[half:]], axis=0))
        upper = even + odd
        lower = even - odd
        back_r = jnp.concatenate([upper[:half], lower[:half]], axis=0)
        back_i = jnp.concatenate([upper[half:], lower[half:]], axis=0)
        term_r = probe_r * back_r + probe_i * back_i
        term_i = probe_r * back_i - probe_i * back_r
        for part, term in ((0, term_r), (1, term_i)):
            grad_ref[(part, *there)] += moved_down(moved_right(term, shift), drop)


def in_order(counts, intensity, order):
    slots, size, _ = intensity.shape
    return pl.pallas_call(
        order_kernel,
        out_shape=jax.ShapeDtypeStruct((slots, size, size), jnp.float32),
        in_specs=[pl.BlockSpec(memory_space=pltpu.SMEM)] + [pl.BlockSpec(memory_space=pltpu.VMEM)] * 2,
        out_specs=pl.BlockSpec(memory_space=pltpu.VMEM),
        cost_estimate=pl.CostEstimate(
            flops=slots * 4 * size**3, bytes_accessed=slots * 8 * size**2, transcendentals=0
        ),
        compiler_params=pltpu.CompilerParams(vmem_limit_bytes=12 * 1024 * 1024),
        name="order",
    )(counts, order, intensity)


def slot_terms(positions, counts, padded, probe, measured, table):
    slots, size, _ = measured.shape
    return pl.pallas_call(
        slots_kernel,
        out_shape=jax.ShapeDtypeStruct(padded.shape, jnp.float32),
        in_specs=[pl.BlockSpec(memory_space=pltpu.SMEM)] * 2 + [pl.BlockSpec(memory_space=pltpu.VMEM)] * 4,
        out_specs=pl.BlockSpec(memory_space=pltpu.VMEM),
        cost_estimate=pl.CostEstimate(
            flops=slots * 48 * size**3, bytes_accessed=slots * 40 * size**2, transcendentals=0
        ),
        compiler_params=pltpu.CompilerParams(vmem_limit_bytes=20 * 1024 * 1024),
        name="slots",
    )(positions, counts, padded, probe, measured, table)


MESH = pl.DeviceIdType.MESH


class Around:
    def __init__(self, send_sems, recv_sems):
        self.send_sems, self.recv_sems = send_sems, recv_sems
        self.sends = self.recvs = 0
        self.here, self.device = {}, {}
        for axis in ("rows", "cols"):
            count = lax.axis_size(axis)
            me = lax.axis_index(axis)
            for d in (-2, -1, 1, 2):
                self.here[axis, d] = me + d >= 0 if d < 0 else me + d < count
                self.device[axis, d] = {axis: lax.rem(me + count + d, count)}
        count = lax.axis_size("rows")
        self.relays = count > 2 and count % 2 == 0
        odd = lax.rem(lax.axis_index("rows"), 2) == 1
        self.far = {1: odd, -1: no(odd)}

    def meet(self):
        barrier = pltpu.get_barrier_semaphore()
        sides = [("rows", -1), ("rows", 1), ("cols", -1), ("cols", 1)]
        if self.relays:
            sides += [("rows", -2), ("rows", 2)]
        for side in sides:

            @pl.when(self.here[side])
            def _():
                pl.semaphore_signal(barrier, inc=1, device_id=self.device[side], device_id_type=MESH)

        pl.semaphore_wait(barrier, sum(self.here[side].astype(jnp.int32) for side in sides))

    def new_recv(self):
        self.recvs += 1
        return self.recvs - 1

    def copy(self, side, source, target, recv=None):
        recv = self.new_recv() if recv is None else recv
        self.sends += 1
        return pltpu.make_async_remote_copy(
            src_ref=source,
            dst_ref=target,
            send_sem=self.send_sems.at[self.sends - 1],
            recv_sem=self.recv_sems.at[recv],
            device_id=self.device[side],
            device_id_type=MESH,
        )


class Side:
    def __init__(self, around, axis, d, source, target):
        self.here, self.back = around.here[axis, d], around.here[axis, -d]
        self.straight = around.copy((axis, d), source, target)

    def start(self):
        pl.when(self.here)(self.straight.start)

    def wait_recv(self):
        pl.when(self.back)(self.straight.wait_recv)

    def wait_send(self):
        pl.when(self.here)(self.straight.wait_send)


class Hop:
    def __init__(self, around, d, source, target, relay):
        here, far = around.here["rows", d], around.far[d]
        self.back = around.here["rows", -d]
        recv = around.new_recv()
        self.straight = around.copy(("rows", d), source, target, recv)
        self.near = both(here, no(far))
        self.long = both(here, far)
        self.middle = both(around.here["rows", -2 * d], far)
        self.first = around.copy(("rows", 2 * d), source, relay)
        self.second = around.copy(("rows", -d), relay, target, recv)

    def start(self):
        pl.when(self.near)(self.straight.start)
        pl.when(self.long)(self.first.start)

    def forward(self):
        @pl.when(self.middle)
        def _():
            self.first.wait_recv()
            self.second.start()

    def wait_recv(self):
        pl.when(self.back)(self.straight.wait_recv)

    def wait_send(self):
        pl.when(self.near)(self.straight.wait_send)
        pl.when(self.long)(self.first.wait_send)
        pl.when(self.middle)(self.second.wait_send)


def both(first, second):
    return jnp.logical_and(first, second)


def no(flag):
    return jnp.logical_not(flag)


def pad_kernel(field_ref, out_ref, relay_ref, send_sems, recv_sems):
    m = MARGIN
    planes, high, wide = field_ref.shape
    around = Around(send_sems, recv_sems)
    here = around.here
    around.meet()
    row_cuts = {-1: (pl.ds(0, m), pl.ds(m + high, m)), 1: (pl.ds(high - m, m), pl.ds(0, m))}
    col_cuts = {-1: (pl.ds(0, m), pl.ds(m + wide, m)), 1: (pl.ds(wide - m, m), pl.ds(0, m))}
    from_cuts = {-1: pl.ds(0, m), 1: pl.ds(m + high, m)}
    col_from = {-1: pl.ds(m, m), 1: pl.ds(wide, m)}
    rows, cols, corners = {}, {}, {}
    for p in range(planes):
        for d in (-1, 1):
            cut, land = row_cuts[d]
            source, target = field_ref.at[p, cut, :], out_ref.at[p, land, pl.ds(m, wide)]
            if around.relays and p == 0:
                rows[p, d] = Hop(around, d, source, target, relay_ref.at[0, 0])
            else:
                rows[p, d] = Side(around, "rows", d, source, target)
            cut, land = col_cuts[d]
            cols[p, d] = Side(around, "cols", d, field_ref.at[p, :, cut], out_ref.at[p, pl.ds(m, high), land])
            for v in (-1, 1):
                corners[p, v, d] = around.copy(
                    ("cols", d), out_ref.at[p, from_cuts[v], col_from[d]], out_ref.at[p, from_cuts[v], land]
                )
    for p in range(planes):
        for d in (-1, 1):
            rows[p, d].start()
    for p in range(planes):
        for d in (-1, 1):
            cols[p, d].start()
    out_ref[:, m : m + high, m : m + wide] = field_ref[...]
    for v in (-1, 1):

        @pl.when(no(here["rows", v]))
        def _():
            out_ref[:, from_cuts[v], m : m + wide] = jnp.zeros((planes, m, wide), jnp.float32)

        for d in (-1, 1):
            land = col_cuts[-d][1]

            @pl.when(no(both(here["rows", v], here["cols", d])))
            def _():
                out_ref[:, from_cuts[v], land] = jnp.zeros((planes, m, m), jnp.float32)

    for d in (-1, 1):
        land = col_cuts[-d][1]

        @pl.when(no(here["cols", d]))
        def _():
            out_ref[:, m : m + high, land] = jnp.zeros((planes, high, m), jnp.float32)

    if around.relays:
        for d in (-1, 1):
            rows[0, d].forward()
    for p in reversed(range(planes)):
        for v in (-1, 1):
            rows[p, -v].wait_recv()
            for d in (-1, 1):
                pl.when(both(here["rows", v], here["cols", d]))(corners[p, v, d].start)
    for p in range(planes):
        for d in (-1, 1):
            cols[p, -d].wait_recv()
            for v in (-1, 1):
                pl.when(both(here["rows", v], here["cols", d]))(corners[p, v, -d].wait_recv)
    for p in range(planes):
        for d in (-1, 1):
            rows[p, d].wait_send()
            cols[p, d].wait_send()
            for v in (-1, 1):
                pl.when(both(here["rows", v], here["cols", d]))(corners[p, v, d].wait_send)


def step_kernel(last, grad_ref, padded_ref, out_ref, mid_ref, side_ref, band_ref, relay_ref, send_sems, recv_sems):
    m = MARGIN
    planes, extent, _ = grad_ref.shape
    wide = extent - 2 * m
    part = extent // 4
    around = Around(send_sems, recv_sems)
    here = around.here
    around.meet()
    begin = {(-1, 0): 0, (-1, 1): part, (1, 1): 2 * part, (1, 0): 3 * part}
    lines = {key: pl.ds(start, part) for key, start in begin.items()}
    cut = {-1: pl.ds(0, m), 1: pl.ds(extent - m, m)}
    inner = {-1: pl.ds(m, m), 1: pl.ds(wide, m)}
    blocks = {q: [(p, h, q) for p in range(planes) for h in (-1, 1)] for q in (0, 1)}
    sides, bands, edges = {}, {}, {}
    for p, h, q in blocks[0] + blocks[1]:
        for d in (-1, 1):
            slot = (d + 1) // 2
            sides[p, h, q, d] = Side(
                around, "cols", d, grad_ref.at[p, lines[h, q], cut[d]], side_ref.at[slot, p, lines[h, q]]
            )
            if not last:
                edges[p, h, q, d] = Side(
                    around, "cols", d, out_ref.at[p, lines[h, q], inner[d]], out_ref.at[p, lines[h, q], cut[-d]]
                )
        if last and q == 1:
            continue
        source, target = mid_ref.at[p, lines[h, q]], band_ref.at[p, lines[-h, 1 - q]]
        if around.relays and (p == 0 if last else q == 0):
            bands[p, h, q] = Hop(around, h, source, target, relay_ref.at[p, 0])
        else:
            bands[p, h, q] = Side(around, "rows", h, source, target)
    for key in sides:
        sides[key].start()
    if not last:
        for d in (-1, 1):

            @pl.when(no(here["cols", d]))
            def _():
                out_ref[:, :, cut[d]] = jnp.zeros((planes, extent, m), jnp.float32)

    for p, h, q in blocks[0] + blocks[1]:
        mid_ref[p, lines[h, q]] = grad_ref[p, lines[h, q], m : m + wide]
        for d in (-1, 1):
            slot = (1 - d) // 2
            target = pl.ds(0, m) if d < 0 else pl.ds(wide - m, m)

            @pl.when(here["cols", d])
            def _():
                sides[p, h, q, -d].straight.wait_recv()
                mid_ref[p, lines[h, q], target] += side_ref[slot, p, lines[h, q]]

        if (p, h, q) in bands:
            bands[p, h, q].start()
    for band in bands.values():
        if isinstance(band, Hop):
            band.forward()
    for p, h, q in blocks[0] + blocks[1]:
        rows = lines[h, q]
        if last and q == 0:
            continue

        @pl.when(here["rows", h])
        def _():
            bands[p, -h, 1 - q].straight.wait_recv()
            total = mid_ref[p, rows] + band_ref[p, rows]
            value = padded_ref[p, rows, m : m + wide] - step_rate * total
            if last:
                out_ref[p, pl.ds(rows.start - m, part)] = value
            else:
                out_ref[p, rows, m : m + wide] = value

        @pl.when(no(here["rows", h]))
        def _():
            if q == 0:
                out_ref[p, rows, m : m + wide] = jnp.zeros((part, wide), jnp.float32)
            else:
                value = padded_ref[p, rows, m : m + wide] - step_rate * mid_ref[p, rows]
                if last:
                    out_ref[p, pl.ds(rows.start - m, part)] = value
                else:
                    out_ref[p, rows, m : m + wide] = value

        if not last:
            for d in (-1, 1):
                edges[p, h, q, d].start()
    for edge in edges.values():
        edge.wait_recv()
    for copy in [*edges.values(), *sides.values(), *bands.values()]:
        copy.wait_send()


def exchange(kernel, name, collective_id, shape, scratch, copies, *arrays):
    return pl.pallas_call(
        kernel,
        out_shape=jax.ShapeDtypeStruct(shape, jnp.float32),
        in_specs=[pl.BlockSpec(memory_space=pltpu.VMEM)] * len(arrays),
        out_specs=pl.BlockSpec(memory_space=pltpu.VMEM),
        scratch_shapes=[pltpu.VMEM(s, jnp.float32) for s in scratch]
        + [pltpu.SemaphoreType.DMA((copies,)), pltpu.SemaphoreType.DMA((copies,))],
        compiler_params=pltpu.CompilerParams(
            collective_id=collective_id, has_side_effects=True, vmem_limit_bytes=12 * 1024 * 1024
        ),
        name=name,
    )(*arrays)


def on_device(object_field, probe, positions, counts, intensity):
    planes, high, wide = object_field.shape
    size = probe.shape[1]
    table = jnp.asarray(tables(size))
    order = jnp.asarray(ordering(size))
    measured = in_order(counts, intensity[0, 0], order)
    tall, broad = high + 2 * MARGIN, wide + 2 * MARGIN
    outer = (planes, tall, broad)
    relay = (planes, 2, MARGIN, wide)
    scratch = [(planes, tall, wide), (2, planes, tall, MARGIN), (planes, tall, wide), relay]
    padded = exchange(pad_kernel, "pad", 0, outer, [relay], 16 * planes, object_field)
    for step in range(ITERS):
        grad = slot_terms(positions, counts, padded, probe, measured, table)
        last = step == ITERS - 1
        kernel = functools.partial(step_kernel, last)
        shape = object_field.shape if last else outer
        padded = exchange(kernel, "step", 1 + step, shape, scratch, 32 * planes, grad, padded)
    return padded


def solution(mesh):
    placed = (
        P(None, "rows", "cols"),
        P(),
        P("rows", "cols", None, None),
        P("rows", "cols"),
        P("rows", "cols", None, None, None),
    )
    return jax.shard_map(
        on_device, mesh=mesh, in_specs=placed, out_specs=P(None, "rows", "cols"), check_vma=False
    )
```

```python
import functools

import jax
import jax.numpy as jnp
import numpy as np
from jax import lax
from jax.experimental import pallas as pl
from jax.experimental.pallas import tpu as pltpu
from jax.sharding import PartitionSpec as P

MARGIN = 128
ITERS = 2
LANES = 128
ROWS = 8
PAIR = 2


step_rate = 0.02
photon_unit = 0.001


def tables(length):
    half = length // 2
    k = np.arange(half)[:, None]
    n = np.arange(half)[None, :]
    found = []
    for odd in (0, 1):
        angle = ((2 * k + odd) * n % length) * (2.0 * np.pi / length)
        c = np.cos(angle) / np.sqrt(length)
        s = np.sin(angle) / np.sqrt(length)
        full = np.block([[c, s], [-s, c]])
        found += [full, full.T]
    full = np.stack(found).astype(np.float32)
    high = full.astype(jnp.bfloat16)
    low = (full - high.astype(np.float32)).astype(jnp.bfloat16)
    return np.stack([high, low])


def dot(left, right):
    return lax.dot_general(left, right, (((1,), (0,)), ((), ())), preferred_element_type=jnp.float32)


def parted(value):
    high = value.astype(jnp.bfloat16)
    return high, (value - high.astype(jnp.float32)).astype(jnp.bfloat16)


def order_columns(length):
    half = length // 2
    here = lax.broadcasted_iota(jnp.int32, (length, length), 0)
    there = lax.broadcasted_iota(jnp.int32, (length, length), 1)
    wanted = jnp.where(there < half, 2 * there, 2 * there - length + 1)
    return jnp.where(here == wanted, 1.0, 0.0).astype(jnp.bfloat16)


def put_in_order(raw_ref, measured_ref, order):
    parts, size, _ = raw_ref.shape
    given = jnp.concatenate(
        [
            jnp.concatenate([raw_ref[c, pl.ds(odd, size // 2, stride=2)] for c in range(parts)], axis=1)
            for odd in (0, 1)
        ],
        axis=0,
    )

    def placed(value):
        return dot(value.astype(jnp.float32).astype(jnp.bfloat16), order)

    measured_ref[...] = (placed(given >> 4) * 16.0 + placed(given & 15)) * photon_unit


def from_left(table, which, value):
    high, low = value
    table = jnp.concatenate([table[0, which], table[1, which], table[0, which]], axis=1)
    return dot(table, jnp.concatenate([high, high, low], axis=0))


def from_right(table, which, value):
    high, low = value
    table = jnp.concatenate([table[0, which], table[1, which], table[0, which]], axis=0)
    return dot(jnp.concatenate([high, high, low], axis=1), table)


def turned(value, drop, shift):
    rows, columns = value.shape
    groups = pltpu.roll(value.reshape(rows // ROWS, ROWS, columns), drop % ROWS, 1)
    before = jnp.concatenate([groups[-1:], groups[:-1]], axis=0)
    within = lax.broadcasted_iota(jnp.int32, (1, ROWS, columns), 1) >= drop
    value = jnp.where(within, groups, before).reshape(rows, columns)
    parts = [pltpu.roll(value[:, c : c + LANES], shift % LANES, 1) for c in range(0, columns, LANES)]
    within = lax.broadcasted_iota(jnp.int32, (rows, LANES), 1) >= shift
    return jnp.concatenate([jnp.where(within, a, b) for a, b in zip(parts, parts[-1:] + parts[:-1])], axis=1)


def wrapped(value, drop, shift):
    rows, columns = value.shape[0] - ROWS, value.shape[1] - LANES
    below = lax.broadcasted_iota(jnp.int32, (ROWS, columns + LANES), 0) >= drop
    value = jnp.concatenate([jnp.where(below, value[:ROWS], value[rows:]), value[ROWS:rows]], axis=0)
    beside = lax.broadcasted_iota(jnp.int32, (rows, LANES), 1) >= shift
    return jnp.concatenate([jnp.where(beside, value[:, :LANES], value[:, columns:]), value[:, LANES:columns]], axis=1)


def unwrapped(value, drop, shift):
    rows, columns = value.shape
    head = value[:, :LANES]
    none = jnp.zeros_like(head)
    beside = lax.broadcasted_iota(jnp.int32, (rows, LANES), 1) >= shift
    value = jnp.concatenate(
        [jnp.where(beside, head, none), value[:, LANES:], jnp.where(beside, none, head)], axis=1
    )
    head = value[:ROWS]
    none = jnp.zeros_like(head)
    below = lax.broadcasted_iota(jnp.int32, (ROWS, columns + LANES), 0) >= drop
    return jnp.concatenate(
        [jnp.where(below, head, none), value[ROWS:], jnp.where(below, none, head)], axis=0
    )


def slot_stages(slot, positions_ref, padded_ref, probe_ref, measured_ref, table_ref, grad_ref):
    size = probe_ref.shape[1]
    half = size // 2
    last = padded_ref.shape[1] - size - ROWS
    row = positions_ref[0, slot]
    column = positions_ref[1, slot]
    start = pl.multiple_of(jnp.where(column >= LANES, LANES, 0), LANES)
    shift = column - start
    first = pl.multiple_of(jnp.minimum(row // ROWS * ROWS, last), ROWS)
    drop = row - first
    there = (pl.ds(first, size + ROWS), pl.ds(start, size + LANES))
    probe_r = turned(probe_ref[0], drop, shift)
    probe_i = turned(probe_ref[1], drop, shift)
    yield
    patch_r = wrapped(padded_ref[(0, *there)], drop, shift)
    patch_i = wrapped(padded_ref[(1, *there)], drop, shift)
    exit_r = probe_r * patch_r - probe_i * patch_i
    exit_i = probe_r * patch_i + probe_i * patch_r
    upper = jnp.concatenate([exit_r[:half], exit_i[:half]], axis=0)
    lower = jnp.concatenate([exit_r[half:], exit_i[half:]], axis=0)
    even, odd = parted(upper + lower), parted(upper - lower)
    yield
    even, odd = from_left(table_ref, 0, even), from_left(table_ref, 2, odd)
    yield
    half_r = jnp.concatenate([even[:half], odd[:half]], axis=0)
    half_i = jnp.concatenate([even[half:], odd[half:]], axis=0)
    left = jnp.concatenate([half_r[:, :half], half_i[:, :half]], axis=1)
    right = jnp.concatenate([half_r[:, half:], half_i[:, half:]], axis=1)
    values = [parted(left + right), parted(left - right)]
    yield
    specs = [from_right(table_ref, 2 * odd + 1, value) for odd, value in enumerate(values)]
    yield
    values = []
    for odd, spec in enumerate(specs):
        spec_r, spec_i = spec[:, :half], spec[:, half:]
        misfit = spec_r * spec_r + spec_i * spec_i - measured_ref[slot, :, odd * half : (odd + 1) * half]
        values.append(parted(jnp.concatenate([misfit * spec_r, misfit * spec_i], axis=1)))
    yield
    backs = [from_right(table_ref, 2 * odd, value) for odd, value in enumerate(values)]
    yield
    left = backs[0] + backs[1]
    right = backs[0] - backs[1]
    half_r = jnp.concatenate([left[:, :half], right[:, :half]], axis=1)
    half_i = jnp.concatenate([left[:, half:], right[:, half:]], axis=1)
    even = parted(jnp.concatenate([half_r[:half], half_i[:half]], axis=0))
    odd = parted(jnp.concatenate([half_r[half:], half_i[half:]], axis=0))
    yield
    even, odd = from_left(table_ref, 1, even), from_left(table_ref, 3, odd)
    yield
    upper = even + odd
    lower = even - odd
    back_r = jnp.concatenate([upper[:half], lower[:half]], axis=0)
    back_i = jnp.concatenate([upper[half:], lower[half:]], axis=0)
    term_r = probe_r * back_r + probe_i * back_i
    term_i = probe_r * back_i - probe_i * back_r
    for part, term in ((0, term_r), (1, term_i)):
        grad_ref[(part, *there)] += unwrapped(term, drop, shift)


def side_by_side(works):
    works = list(works)
    while works:
        works = [work for work in works if next(work, works) is not works]


def slots_kernel(positions_ref, counts_ref, padded_ref, *refs):
    grad_ref = refs[-1]
    count = counts_ref[0, 0]
    grad_ref[...] = jnp.zeros_like(grad_ref)

    def work(slot):
        return slot_stages(slot, positions_ref, padded_ref, *refs)

    @pl.loop(0, count // PAIR)
    def _(group):
        side_by_side(work(group * PAIR + k) for k in range(PAIR))

    @pl.loop(count // PAIR * PAIR, count)
    def _(slot):
        side_by_side([work(slot)])


def slot_terms(positions, counts, padded, probe, measured, table):
    slots, size, _ = measured.shape
    return pl.pallas_call(
        slots_kernel,
        out_shape=jax.ShapeDtypeStruct(padded.shape, jnp.float32),
        in_specs=[pl.BlockSpec(memory_space=pltpu.SMEM)] * 2 + [pl.BlockSpec(memory_space=pltpu.VMEM)] * 4,
        out_specs=pl.BlockSpec(memory_space=pltpu.VMEM),
        cost_estimate=pl.CostEstimate(
            flops=slots * 48 * size**3, bytes_accessed=slots * 40 * size**2, transcendentals=0
        ),
        compiler_params=pltpu.CompilerParams(vmem_limit_bytes=20 * 1024 * 1024),
        name="slots",
    )(positions, counts, padded, probe, measured, table)


MESH = pl.DeviceIdType.MESH


class Around:
    def __init__(self, send_sems, recv_sems):
        self.send_sems, self.recv_sems = send_sems, recv_sems
        self.sends = self.recvs = 0
        self.here, self.device = {}, {}
        for axis in ("rows", "cols"):
            count = lax.axis_size(axis)
            me = lax.axis_index(axis)
            for d in (-2, -1, 1, 2):
                self.here[axis, d] = me + d >= 0 if d < 0 else me + d < count
                self.device[axis, d] = {axis: lax.rem(me + count + d, count)}
        count = lax.axis_size("rows")
        self.relays = count > 2 and count % 2 == 0
        odd = lax.rem(lax.axis_index("rows"), 2) == 1
        self.far = {1: odd, -1: no(odd)}

    def meet(self):
        barrier = pltpu.get_barrier_semaphore()
        sides = [("rows", -1), ("rows", 1), ("cols", -1), ("cols", 1)]
        if self.relays:
            sides += [("rows", -2), ("rows", 2)]
        for side in sides:

            @pl.when(self.here[side])
            def _():
                pl.semaphore_signal(barrier, inc=1, device_id=self.device[side], device_id_type=MESH)

        pl.semaphore_wait(barrier, sum(self.here[side].astype(jnp.int32) for side in sides))

    def new_recv(self):
        self.recvs += 1
        return self.recvs - 1

    def copy(self, side, source, target, recv=None):
        recv = self.new_recv() if recv is None else recv
        self.sends += 1
        return pltpu.make_async_remote_copy(
            src_ref=source,
            dst_ref=target,
            send_sem=self.send_sems.at[self.sends - 1],
            recv_sem=self.recv_sems.at[recv],
            device_id=self.device[side],
            device_id_type=MESH,
        )


class Side:
    def __init__(self, around, axis, d, source, target):
        self.here, self.back = around.here[axis, d], around.here[axis, -d]
        self.straight = around.copy((axis, d), source, target)

    def start(self):
        pl.when(self.here)(self.straight.start)

    def wait_recv(self):
        pl.when(self.back)(self.straight.wait_recv)

    def wait_send(self):
        pl.when(self.here)(self.straight.wait_send)


class Hop:
    def __init__(self, around, d, source, target, relay):
        here, far = around.here["rows", d], around.far[d]
        self.back = around.here["rows", -d]
        recv = around.new_recv()
        self.straight = around.copy(("rows", d), source, target, recv)
        self.near = both(here, no(far))
        self.long = both(here, far)
        self.middle = both(around.here["rows", -2 * d], far)
        self.first = around.copy(("rows", 2 * d), source, relay)
        self.second = around.copy(("rows", -d), relay, target, recv)

    def start(self):
        pl.when(self.near)(self.straight.start)
        pl.when(self.long)(self.first.start)

    def forward(self):
        @pl.when(self.middle)
        def _():
            self.first.wait_recv()
            self.second.start()

    def wait_recv(self):
        pl.when(self.back)(self.straight.wait_recv)

    def wait_send(self):
        pl.when(self.near)(self.straight.wait_send)
        pl.when(self.long)(self.first.wait_send)
        pl.when(self.middle)(self.second.wait_send)


def both(first, second):
    return jnp.logical_and(first, second)


def no(flag):
    return jnp.logical_not(flag)


def pad_kernel(
    field_ref, intensity_ref, out_ref, measured_ref, relay_ref, raw_ref, send_sems, recv_sems, local_sems
):
    m = MARGIN
    planes, high, wide = field_ref.shape
    slots, size, _ = measured_ref.shape
    own = pltpu.make_async_copy(field_ref, out_ref.at[:, pl.ds(m, high), pl.ds(m, wide)], local_sems.at[slots * (size // LANES)])
    own.start()
    parts = size // LANES
    fetches = [
        pltpu.make_async_copy(
            intensity_ref.at[0, 0, k, :, pl.ds(c * LANES, LANES)], raw_ref.at[k, c], local_sems.at[k * parts + c]
        )
        for k in range(slots)
        for c in range(parts)
    ]
    for fetch in fetches:
        fetch.start()
    around = Around(send_sems, recv_sems)
    here = around.here
    around.meet()
    row_cuts = {-1: (pl.ds(0, m), pl.ds(m + high, m)), 1: (pl.ds(high - m, m), pl.ds(0, m))}
    col_cuts = {-1: (pl.ds(0, m), pl.ds(m + wide, m)), 1: (pl.ds(wide - m, m), pl.ds(0, m))}
    from_cuts = {-1: pl.ds(0, m), 1: pl.ds(m + high, m)}
    col_from = {-1: pl.ds(m, m), 1: pl.ds(wide, m)}
    rows, cols, corners = {}, {}, {}
    for p in range(planes):
        for d in (-1, 1):
            cut, land = row_cuts[d]
            source, target = field_ref.at[p, cut, :], out_ref.at[p, land, pl.ds(m, wide)]
            if around.relays and p == 0:
                rows[p, d] = Hop(around, d, source, target, relay_ref.at[0, 0])
            else:
                rows[p, d] = Side(around, "rows", d, source, target)
            cut, land = col_cuts[d]
            cols[p, d] = Side(around, "cols", d, field_ref.at[p, :, cut], out_ref.at[p, pl.ds(m, high), land])
            for v in (-1, 1):
                corners[p, v, d] = around.copy(
                    ("cols", d), out_ref.at[p, from_cuts[v], col_from[d]], out_ref.at[p, from_cuts[v], land]
                )
    for p in range(planes):
        for d in (-1, 1):
            rows[p, d].start()
    for p in range(planes):
        for d in (-1, 1):
            cols[p, d].start()
    for v in (-1, 1):

        @pl.when(no(here["rows", v]))
        def _():
            out_ref[:, from_cuts[v], m : m + wide] = jnp.zeros((planes, m, wide), jnp.float32)

        for d in (-1, 1):
            land = col_cuts[-d][1]

            @pl.when(no(both(here["rows", v], here["cols", d])))
            def _():
                out_ref[:, from_cuts[v], land] = jnp.zeros((planes, m, m), jnp.float32)

    for d in (-1, 1):
        land = col_cuts[-d][1]

        @pl.when(no(here["cols", d]))
        def _():
            out_ref[:, m : m + high, land] = jnp.zeros((planes, high, m), jnp.float32)

    order = order_columns(size)
    for k in range(slots):
        for c in range(parts):
            fetches[k * parts + c].wait()
        put_in_order(raw_ref.at[k], measured_ref.at[k], order)
    if around.relays:
        for d in (-1, 1):
            rows[0, d].forward()
    for p in reversed(range(planes)):
        for v in (-1, 1):
            rows[p, -v].wait_recv()
            for d in (-1, 1):
                pl.when(both(here["rows", v], here["cols", d]))(corners[p, v, d].start)
    for p in range(planes):
        for d in (-1, 1):
            cols[p, -d].wait_recv()
            for v in (-1, 1):
                pl.when(both(here["rows", v], here["cols", d]))(corners[p, v, -d].wait_recv)
    for p in range(planes):
        for d in (-1, 1):
            rows[p, d].wait_send()
            cols[p, d].wait_send()
            for v in (-1, 1):
                pl.when(both(here["rows", v], here["cols", d]))(corners[p, v, d].wait_send)
    own.wait()


def step_kernel(last, grad_ref, padded_ref, out_ref, mid_ref, side_ref, band_ref, relay_ref, send_sems, recv_sems):
    m = MARGIN
    planes, extent, _ = grad_ref.shape
    wide = extent - 2 * m
    part = extent // 4
    around = Around(send_sems, recv_sems)
    here = around.here
    around.meet()
    begin = {(-1, 0): 0, (-1, 1): part, (1, 1): 2 * part, (1, 0): 3 * part}
    lines = {key: pl.ds(start, part) for key, start in begin.items()}
    cut = {-1: pl.ds(0, m), 1: pl.ds(extent - m, m)}
    inner = {-1: pl.ds(m, m), 1: pl.ds(wide, m)}
    blocks = {q: [(p, h, q) for p in range(planes) for h in (-1, 1)] for q in (0, 1)}
    sides, bands, edges = {}, {}, {}
    for p, h, q in blocks[0] + blocks[1]:
        for d in (-1, 1):
            slot = (d + 1) // 2
            sides[p, h, q, d] = Side(
                around, "cols", d, grad_ref.at[p, lines[h, q], cut[d]], side_ref.at[slot, p, lines[h, q]]
            )
            if not last:
                edges[p, h, q, d] = Side(
                    around, "cols", d, out_ref.at[p, lines[h, q], inner[d]], out_ref.at[p, lines[h, q], cut[-d]]
                )
        if last and q == 1:
            continue
        source, target = mid_ref.at[p, lines[h, q]], band_ref.at[p, lines[-h, 1 - q]]
        if around.relays and (p == 0 if last else q == 0):
            bands[p, h, q] = Hop(around, h, source, target, relay_ref.at[p, 0])
        else:
            bands[p, h, q] = Side(around, "rows", h, source, target)
    for key in sides:
        sides[key].start()
    if not last:
        for d in (-1, 1):

            @pl.when(no(here["cols", d]))
            def _():
                out_ref[:, :, cut[d]] = jnp.zeros((planes, extent, m), jnp.float32)

    for p, h, q in blocks[0] + blocks[1]:
        mid_ref[p, lines[h, q]] = grad_ref[p, lines[h, q], m : m + wide]
        for d in (-1, 1):
            slot = (1 - d) // 2
            target = pl.ds(0, m) if d < 0 else pl.ds(wide - m, m)

            @pl.when(here["cols", d])
            def _():
                sides[p, h, q, -d].straight.wait_recv()
                mid_ref[p, lines[h, q], target] += side_ref[slot, p, lines[h, q]]

        if (p, h, q) in bands:
            bands[p, h, q].start()
    for band in bands.values():
        if isinstance(band, Hop):
            band.forward()
    for p, h, q in blocks[0] + blocks[1]:
        rows = lines[h, q]
        if last and q == 0:
            continue

        @pl.when(here["rows", h])
        def _():
            bands[p, -h, 1 - q].straight.wait_recv()
            total = mid_ref[p, rows] + band_ref[p, rows]
            value = padded_ref[p, rows, m : m + wide] - step_rate * total
            if last:
                out_ref[p, pl.ds(rows.start - m, part)] = value
            else:
                out_ref[p, rows, m : m + wide] = value

        @pl.when(no(here["rows", h]))
        def _():
            if q == 0:
                out_ref[p, rows, m : m + wide] = jnp.zeros((part, wide), jnp.float32)
            else:
                value = padded_ref[p, rows, m : m + wide] - step_rate * mid_ref[p, rows]
                if last:
                    out_ref[p, pl.ds(rows.start - m, part)] = value
                else:
                    out_ref[p, rows, m : m + wide] = value

        if not last:
            for d in (-1, 1):
                edges[p, h, q, d].start()
    for edge in edges.values():
        edge.wait_recv()
    for copy in [*edges.values(), *sides.values(), *bands.values()]:
        copy.wait_send()


def exchange(kernel, name, collective_id, shape, scratch, copies, *arrays):
    return pl.pallas_call(
        kernel,
        out_shape=jax.ShapeDtypeStruct(shape, jnp.float32),
        in_specs=[pl.BlockSpec(memory_space=pltpu.VMEM)] * len(arrays),
        out_specs=pl.BlockSpec(memory_space=pltpu.VMEM),
        scratch_shapes=[pltpu.VMEM(s, jnp.float32) for s in scratch]
        + [pltpu.SemaphoreType.DMA((copies,)), pltpu.SemaphoreType.DMA((copies,))],
        compiler_params=pltpu.CompilerParams(
            collective_id=collective_id, has_side_effects=True, vmem_limit_bytes=12 * 1024 * 1024
        ),
        name=name,
    )(*arrays)


def pad_and_order(field, intensity, relay):
    planes, high, wide = field.shape
    slots, size, _ = intensity.shape[2:]
    copies = 16 * planes
    return pl.pallas_call(
        pad_kernel,
        out_shape=[
            jax.ShapeDtypeStruct((planes, high + 2 * MARGIN, wide + 2 * MARGIN), jnp.float32),
            jax.ShapeDtypeStruct((slots, size, size), jnp.float32),
        ],
        in_specs=[pl.BlockSpec(memory_space=pltpu.HBM)] * 2,
        out_specs=[pl.BlockSpec(memory_space=pltpu.VMEM)] * 2,
        scratch_shapes=[
            pltpu.VMEM(relay, jnp.float32),
            pltpu.VMEM((slots, size // LANES, size, LANES), jnp.int32),
            pltpu.SemaphoreType.DMA((copies,)),
            pltpu.SemaphoreType.DMA((copies,)),
            pltpu.SemaphoreType.DMA((slots * (size // LANES) + 1,)),
        ],
        compiler_params=pltpu.CompilerParams(
            collective_id=0, has_side_effects=True, vmem_limit_bytes=16 * 1024 * 1024
        ),
        name="pad",
    )(*(pltpu.with_memory_space_constraint(array, pltpu.HBM) for array in (field, intensity)))


def on_device(object_field, probe, positions, counts, intensity):
    planes, high, wide = object_field.shape
    table = jnp.asarray(tables(probe.shape[1]))
    positions = positions[0, 0].T
    tall, broad = high + 2 * MARGIN, wide + 2 * MARGIN
    outer = (planes, tall, broad)
    relay = (planes, 2, MARGIN, wide)
    scratch = [(planes, tall, wide), (2, planes, tall, MARGIN), (planes, tall, wide), relay]
    padded, measured = pad_and_order(object_field, intensity, relay)
    for step in range(ITERS):
        grad = slot_terms(positions, counts, padded, probe, measured, table)
        last = step == ITERS - 1
        kernel = functools.partial(step_kernel, last)
        shape = object_field.shape if last else outer
        padded = exchange(kernel, "step", 1 + step, shape, scratch, 32 * planes, grad, padded)
    return padded


def solution(mesh):
    placed = (
        P(None, "rows", "cols"),
        P(),
        P("rows", "cols", None, None),
        P("rows", "cols"),
        P("rows", "cols", None, None, None),
    )
    return jax.shard_map(
        on_device, mesh=mesh, in_specs=placed, out_specs=P(None, "rows", "cols"), check_vma=False
    )
```

```python
import functools
import itertools

import jax
import jax.numpy as jnp
import numpy as np
from jax import lax
from jax.experimental import pallas as pl
from jax.experimental.pallas import tpu as pltpu
from jax.sharding import PartitionSpec as P

MARGIN = 128
ITERS = 2
LANES = 128
ROWS = 8
PAIR = 2
BLOCKS = 4


step_rate = 0.02
photon_unit = 0.001


def tables(length):
    half = length // 2
    k = np.arange(half)[:, None]
    n = np.arange(half)[None, :]
    found = []
    for odd in (0, 1):
        angle = ((2 * k + odd) * n % length) * (2.0 * np.pi / length)
        c = np.cos(angle) / np.sqrt(length)
        s = np.sin(angle) / np.sqrt(length)
        full = np.block([[c, s], [-s, c]])
        found += [full, full.T]
    full = np.stack(found).astype(np.float32)
    high = full.astype(jnp.bfloat16)
    low = (full - high.astype(np.float32)).astype(jnp.bfloat16)
    return np.stack([high, low])


def dot(left, right):
    return lax.dot_general(left, right, (((1,), (0,)), ((), ())), preferred_element_type=jnp.float32)


def parted(value):
    high = value.astype(jnp.bfloat16)
    return high, (value - high.astype(jnp.float32)).astype(jnp.bfloat16)


def order_columns(length):
    half = length // 2
    here = lax.broadcasted_iota(jnp.int32, (length, length), 0)
    there = lax.broadcasted_iota(jnp.int32, (length, length), 1)
    wanted = jnp.where(there < half, 2 * there, 2 * there - length + 1)
    return jnp.where(here == wanted, 1.0, 0.0).astype(jnp.bfloat16)


def put_in_order(raw_ref, measured_ref, order):
    parts, size, _ = raw_ref.shape
    given = jnp.concatenate(
        [
            jnp.concatenate([raw_ref[c, pl.ds(odd, size // 2, stride=2)] for c in range(parts)], axis=1)
            for odd in (0, 1)
        ],
        axis=0,
    )

    def placed(value):
        return dot(value.astype(jnp.float32).astype(jnp.bfloat16), order)

    measured_ref[...] = (placed(given >> 4) * 16.0 + placed(given & 15)) * photon_unit


def from_left(table, which, value):
    high, low = value
    table = jnp.concatenate([table[0, which], table[1, which], table[0, which]], axis=1)
    return dot(table, jnp.concatenate([high, high, low], axis=0))


def from_right(table, which, value):
    high, low = value
    table = jnp.concatenate([table[0, which], table[1, which], table[0, which]], axis=0)
    return dot(jnp.concatenate([high, high, low], axis=1), table)


def turned(value, drop, shift):
    rows, columns = value.shape
    groups = pltpu.roll(value.reshape(rows // ROWS, ROWS, columns), drop % ROWS, 1)
    before = jnp.concatenate([groups[-1:], groups[:-1]], axis=0)
    within = lax.broadcasted_iota(jnp.int32, (1, ROWS, columns), 1) >= drop
    value = jnp.where(within, groups, before).reshape(rows, columns)
    parts = [pltpu.roll(value[:, c : c + LANES], shift % LANES, 1) for c in range(0, columns, LANES)]
    within = lax.broadcasted_iota(jnp.int32, (rows, LANES), 1) >= shift
    return jnp.concatenate([jnp.where(within, a, b) for a, b in zip(parts, parts[-1:] + parts[:-1])], axis=1)


def slot_stages(slot, positions_ref, padded_ref, probes_ref, measured_ref, table_ref, terms):
    size = probes_ref.shape[2]
    half = size // 2
    below = lax.broadcasted_iota(jnp.int32, (size, size), 0) >= positions_ref[0, slot]
    beside = lax.broadcasted_iota(jnp.int32, (size, size), 1) >= positions_ref[1, slot]

    def folded(p):
        upper = jnp.where(beside, padded_ref[p, :size, :size], padded_ref[p, :size, size:])
        lower = jnp.where(beside, padded_ref[p, size:, :size], padded_ref[p, size:, size:])
        return jnp.where(below, upper, lower)

    probe_r = probes_ref[slot, 0]
    probe_i = probes_ref[slot, 1]
    patch_r, patch_i = folded(0), folded(1)
    exit_r = probe_r * patch_r - probe_i * patch_i
    exit_i = probe_r * patch_i + probe_i * patch_r
    upper = jnp.concatenate([exit_r[:half], exit_i[:half]], axis=0)
    lower = jnp.concatenate([exit_r[half:], exit_i[half:]], axis=0)
    even, odd = parted(upper + lower), parted(upper - lower)
    yield
    even, odd = from_left(table_ref, 0, even), from_left(table_ref, 2, odd)
    yield
    half_r = jnp.concatenate([even[:half], odd[:half]], axis=0)
    half_i = jnp.concatenate([even[half:], odd[half:]], axis=0)
    left = jnp.concatenate([half_r[:, :half], half_i[:, :half]], axis=1)
    right = jnp.concatenate([half_r[:, half:], half_i[:, half:]], axis=1)
    values = [parted(left + right), parted(left - right)]
    yield
    specs = [from_right(table_ref, 2 * odd + 1, value) for odd, value in enumerate(values)]
    yield
    values = []
    for odd, spec in enumerate(specs):
        spec_r, spec_i = spec[:, :half], spec[:, half:]
        misfit = spec_r * spec_r + spec_i * spec_i - measured_ref[slot, :, odd * half : (odd + 1) * half]
        values.append(parted(jnp.concatenate([misfit * spec_r, misfit * spec_i], axis=1)))
    yield
    backs = [from_right(table_ref, 2 * odd, value) for odd, value in enumerate(values)]
    yield
    left = backs[0] + backs[1]
    right = backs[0] - backs[1]
    half_r = jnp.concatenate([left[:, :half], right[:, :half]], axis=1)
    half_i = jnp.concatenate([left[:, half:], right[:, half:]], axis=1)
    even = parted(jnp.concatenate([half_r[:half], half_i[:half]], axis=0))
    odd = parted(jnp.concatenate([half_r[half:], half_i[half:]], axis=0))
    yield
    even, odd = from_left(table_ref, 1, even), from_left(table_ref, 3, odd)
    yield
    upper = even + odd
    lower = even - odd
    back_r = jnp.concatenate([upper[:half], lower[:half]], axis=0)
    back_i = jnp.concatenate([upper[half:], lower[half:]], axis=0)
    term_r = probe_r * back_r + probe_i * back_i
    term_i = probe_r * back_i - probe_i * back_r
    for term in (term_r, term_i):
        upper, lower = jnp.where(below, term, 0.0), jnp.where(below, 0.0, term)
        terms.append([jnp.where(beside, t, 0.0) if left else jnp.where(beside, 0.0, t) for t in (upper, lower) for left in (1, 0)])


def side_by_side(works):
    works = list(works)
    while works:
        works = [work for work in works if next(work, works) is not works]


def turn_kernel(positions_ref, counts_ref, probe_ref, probes_ref, twice_ref):
    planes, size, _ = probe_ref.shape
    slots = probes_ref.shape[0]
    count = counts_ref[0, 0]

    @pl.loop(0, count)
    def _(slot):
        row = lax.rem(positions_ref[0, slot], size)
        column = lax.rem(positions_ref[1, slot], size)
        drop, shift = lax.rem(row, ROWS), lax.rem(column, LANES)
        first = pl.multiple_of(size - (row - drop), ROWS)
        for p in range(planes):
            value = turned(probe_ref[p], drop, shift)
            parts = [value[:, c : c + LANES] for c in range(0, size, LANES)]
            for k in range(1, size // LANES):
                moved = jnp.concatenate(parts[-k:] + parts[:-k], axis=1)
                value = jnp.where(column // LANES == k, moved, value)
            twice_ref[p, :size] = value
            twice_ref[p, size:] = value
            probes_ref[slot, p] = twice_ref[p, pl.ds(first, size)]

    @pl.loop(count, slots)
    def _(slot):
        probes_ref[slot] = jnp.zeros(probes_ref.shape[1:], jnp.float32)


def add_terms(positions_ref, padded_ref, probes_ref, measured_ref, table_ref, grad_ref):
    planes = padded_ref.shape[0]
    slots, size, _ = measured_ref.shape

    def group(begin, width):
        terms = [[] for _ in range(width)]
        side_by_side(
            slot_stages(begin + k, positions_ref, padded_ref, probes_ref, measured_ref, table_ref, terms[k])
            for k in range(width)
        )
        for p in range(planes):
            for k, (r, c) in enumerate(itertools.product((0, size), (0, size))):
                grad_ref[p, r : r + size, c : c + size] += sum(term[p][k] for term in terms)

    @pl.loop(0, slots // PAIR)
    def _(step):
        group(step * PAIR, PAIR)

    for slot in range(slots // PAIR * PAIR, slots):
        group(slot, 1)


MESH = pl.DeviceIdType.MESH


class Around:
    def __init__(self, send_sems, recv_sems):
        self.send_sems, self.recv_sems = send_sems, recv_sems
        self.sends = self.recvs = 0
        self.here, self.device = {}, {}
        for axis in ("rows", "cols"):
            count = lax.axis_size(axis)
            me = lax.axis_index(axis)
            for d in (-2, -1, 1, 2):
                self.here[axis, d] = me + d >= 0 if d < 0 else me + d < count
                self.device[axis, d] = {axis: lax.rem(me + count + d, count)}
        count = lax.axis_size("rows")
        self.relays = count > 2 and count % 2 == 0
        odd = lax.rem(lax.axis_index("rows"), 2) == 1
        self.far = {1: odd, -1: no(odd)}

    def meet(self):
        barrier = pltpu.get_barrier_semaphore()
        sides = [("rows", -1), ("rows", 1), ("cols", -1), ("cols", 1)]
        if self.relays:
            sides += [("rows", -2), ("rows", 2)]
        for side in sides:

            @pl.when(self.here[side])
            def _():
                pl.semaphore_signal(barrier, inc=1, device_id=self.device[side], device_id_type=MESH)

        pl.semaphore_wait(barrier, sum(self.here[side].astype(jnp.int32) for side in sides))

    def new_recv(self):
        self.recvs += 1
        return self.recvs - 1

    def copy(self, side, source, target, recv=None):
        recv = self.new_recv() if recv is None else recv
        self.sends += 1
        return pltpu.make_async_remote_copy(
            src_ref=source,
            dst_ref=target,
            send_sem=self.send_sems.at[self.sends - 1],
            recv_sem=self.recv_sems.at[recv],
            device_id=self.device[side],
            device_id_type=MESH,
        )


class Side:
    def __init__(self, around, axis, d, source, target):
        self.here, self.back = around.here[axis, d], around.here[axis, -d]
        self.straight = around.copy((axis, d), source, target)

    def start(self):
        pl.when(self.here)(self.straight.start)

    def forward(self):
        pass

    def wait_recv(self):
        pl.when(self.back)(self.straight.wait_recv)

    def wait_left(self):
        pl.when(self.here)(self.straight.wait_send)

    def wait_forwarded(self):
        pass


class Hop:
    def __init__(self, around, d, source, target, relay):
        here, far = around.here["rows", d], around.far[d]
        self.back = around.here["rows", -d]
        recv = around.new_recv()
        self.straight = around.copy(("rows", d), source, target, recv)
        self.near = both(here, no(far))
        self.long = both(here, far)
        self.middle = both(around.here["rows", -2 * d], far)
        self.first = around.copy(("rows", 2 * d), source, relay)
        self.second = around.copy(("rows", -d), relay, target, recv)

    def start(self):
        pl.when(self.near)(self.straight.start)
        pl.when(self.long)(self.first.start)

    def forward(self):
        @pl.when(self.middle)
        def _():
            self.first.wait_recv()
            self.second.start()

    def wait_recv(self):
        pl.when(self.back)(self.straight.wait_recv)

    def wait_left(self):
        pl.when(self.near)(self.straight.wait_send)
        pl.when(self.long)(self.first.wait_send)

    def wait_forwarded(self):
        pl.when(self.middle)(self.second.wait_send)


def both(first, second):
    return jnp.logical_and(first, second)


def no(flag):
    return jnp.logical_not(flag)


def pad(around, field_ref, out_ref, relay_ref, meanwhile):
    m = MARGIN
    planes, high, wide = field_ref.shape
    here = around.here
    part = m // 2
    row_from = {(-1, q): pl.ds(q * part, part) for q in (0, 1)} | {(1, q): pl.ds(high - m + q * part, part) for q in (0, 1)}
    row_land = {(1, q): pl.ds(q * part, part) for q in (0, 1)} | {(-1, q): pl.ds(m + high + q * part, part) for q in (0, 1)}
    col_cuts = {-1: (pl.ds(0, m), pl.ds(m + wide, m)), 1: (pl.ds(wide - m, m), pl.ds(0, m))}
    from_cuts = {-1: pl.ds(0, m), 1: pl.ds(m + high, m)}
    col_from = {-1: pl.ds(m, m), 1: pl.ds(wide, m)}
    rows, cols, corners = {}, {}, {}
    for d in (-1, 1):
        for q in (0, 1):
            source, target = field_ref.at[:, row_from[d, q]], out_ref.at[:, row_land[d, q], pl.ds(m, wide)]
            if around.relays and q == 0:
                rows[d, q] = Hop(around, d, source, target, relay_ref.at[0, :, pl.ds(0, part)])
            else:
                rows[d, q] = Side(around, "rows", d, source, target)
        cut, land = col_cuts[d]
        cols[d] = Side(around, "cols", d, field_ref.at[:, :, cut], out_ref.at[:, pl.ds(m, high), land])
        for v in (-1, 1):
            for q in (0, 1):
                lines = row_land[-v, q]
                corners[v, q, d] = around.copy(("cols", d), out_ref.at[:, lines, col_from[d]], out_ref.at[:, lines, land])
    for q in (0, 1):
        for d in (-1, 1):
            rows[d, q].start()
    for d in (-1, 1):
        cols[d].start()
    for v in (-1, 1):

        @pl.when(no(here["rows", v]))
        def _():
            out_ref[:, from_cuts[v], m : m + wide] = jnp.zeros((planes, m, wide), jnp.float32)

        for d in (-1, 1):
            land = col_cuts[-d][1]

            @pl.when(no(both(here["rows", v], here["cols", d])))
            def _():
                out_ref[:, from_cuts[v], land] = jnp.zeros((planes, m, m), jnp.float32)

    for d in (-1, 1):
        land = col_cuts[-d][1]

        @pl.when(no(here["cols", d]))
        def _():
            out_ref[:, m : m + high, land] = jnp.zeros((planes, high, m), jnp.float32)

    meanwhile()
    for d in (-1, 1):
        rows[d, 0].forward()
    for far in (-1, 1):

        @pl.when(around.far[far])
        def _():
            for v, q in ((-far, 0), (-far, 1), (far, 1), (far, 0)):
                rows[-v, q].wait_recv()
                for d in (-1, 1):
                    pl.when(both(here["rows", v], here["cols", d]))(corners[v, q, d].start)

    for d in (-1, 1):
        cols[-d].wait_recv()
        for v in (-1, 1):
            for q in (0, 1):
                pl.when(both(here["rows", v], here["cols", d]))(corners[v, q, -d].wait_recv)
    def rest():
        for copy in [*rows.values(), *cols.values()]:
            copy.wait_left()
            copy.wait_forwarded()
        for v, q, d in corners:
            pl.when(both(here["rows", v], here["cols", d]))(corners[v, q, d].wait_send)

    return rest


def step(last, around, grad_ref, padded_ref, out_ref, mid_ref, side_ref, band_ref, relay_ref):
    m = MARGIN
    planes, extent, _ = grad_ref.shape
    wide = extent - 2 * m
    part = extent // 2 // BLOCKS
    outside = m // part
    here = around.here
    begin = {(h, q): q * part if h < 0 else extent - (q + 1) * part for h in (-1, 1) for q in range(BLOCKS)}
    lines = {key: pl.ds(start, part) for key, start in begin.items()}
    cut = {-1: pl.ds(0, m), 1: pl.ds(extent - m, m)}
    inner = {-1: pl.ds(m, m), 1: pl.ds(wide, m)}
    sent = range(outside if last else BLOCKS)
    relayed = len(sent) // 2
    sides, bands, edges = {}, {}, {}
    for q in range(BLOCKS):
        for h in (-1, 1):
            for d in (-1, 1):
                sides[h, q, d] = Side(
                    around, "cols", d, grad_ref.at[:, lines[h, q], cut[d]], side_ref.at[(d + 1) // 2, :, lines[h, q]]
                )
                if not last:
                    edges[h, q, d] = Side(
                        around, "cols", d, out_ref.at[:, lines[h, q], inner[d]], out_ref.at[:, lines[h, q], cut[-d]]
                    )
            if q not in sent:
                continue
            source, target = mid_ref.at[:, lines[h, q]], band_ref.at[:, lines[-h, BLOCKS - 1 - q]]
            if around.relays and q < relayed:
                bands[h, q] = Hop(around, h, source, target, relay_ref.at[q, :, pl.ds(0, part)])
            else:
                bands[h, q] = Side(around, "rows", h, source, target)
    for side in sides.values():
        side.start()
    if not last:
        for d in (-1, 1):

            @pl.when(no(here["cols", d]))
            def _():
                out_ref[:, :, cut[d]] = jnp.zeros((planes, extent, m), jnp.float32)

    def gather(h, q):
        mid_ref[:, lines[h, q]] = grad_ref[:, lines[h, q], m : m + wide]
        for d in (-1, 1):
            target = pl.ds(0, m) if d < 0 else pl.ds(wide - m, m)

            @pl.when(here["cols", d])
            def _():
                sides[h, q, -d].straight.wait_recv()
                mid_ref[:, lines[h, q], target] += side_ref[(1 - d) // 2, :, lines[h, q]]

    def finish(h, q):
        rows = lines[h, q]
        place = (slice(None), pl.ds(rows.start - m, part)) if last else (slice(None), rows, slice(m, m + wide))

        @pl.when(here["rows", h])
        def _():
            bands[-h, BLOCKS - 1 - q].straight.wait_recv()
            total = mid_ref[:, rows] + band_ref[:, rows]
            out_ref[place] = padded_ref[:, rows, m : m + wide] - step_rate * total

        @pl.when(no(here["rows", h]))
        def _():
            if q < outside:
                out_ref[place] = jnp.zeros((planes, part, wide), jnp.float32)
            else:
                out_ref[place] = padded_ref[:, rows, m : m + wide] - step_rate * mid_ref[:, rows]

        if not last:
            for d in (-1, 1):
                edges[h, q, d].start()

    def by_parity(work):
        for far in (-1, 1):
            pl.when(around.far[far])(functools.partial(work, far))

    for q in range(BLOCKS):
        for h in (-1, 1):
            gather(h, q)
            if q in sent:
                bands[h, q].start()
    for band in bands.values():
        band.forward()

    def finish_all(far):
        near = [(-far, q) for q in sent]
        order = near[:relayed]
        for q in sent[relayed:]:
            order += [near[q], (far, q)]
        for h, q in order + [(far, q) for q in sent[:relayed]]:
            finish(h, BLOCKS - 1 - q)

    by_parity(finish_all)
    for edge in edges.values():
        edge.wait_recv()
    def rest():
        for copy in [*bands.values(), *edges.values(), *sides.values()]:
            copy.wait_left()
            copy.wait_forwarded()

    return rest


def whole_kernel(
    positions_ref,
    field_ref,
    intensity_ref,
    probes_ref,
    table_from,
    out_ref,
    *refs,
):
    padded_refs, refs = refs[:ITERS], refs[ITERS:]
    work(
        positions_ref, field_ref, intensity_ref, probes_ref, table_from, out_ref, padded_refs, *refs
    )


def work(
    positions_ref,
    field_ref,
    intensity_ref,
    probes_ref,
    table_from,
    out_ref,
    padded_refs,
    grad_ref,
    measured_ref,
    raw_ref,
    table_ref,
    mid_ref,
    side_ref,
    band_ref,
    relay_ref,
    send_sems,
    recv_sems,
    local_sems,
):
    m = MARGIN
    planes, high, wide = field_ref.shape
    slots, size, _ = measured_ref.shape
    parts = size // LANES
    own = pltpu.make_async_copy(
        field_ref, padded_refs[0].at[:, pl.ds(m, high), pl.ds(m, wide)], local_sems.at[slots * parts]
    )
    fetches = [
        pltpu.make_async_copy(
            intensity_ref.at[0, 0, k, :, pl.ds(c * LANES, LANES)], raw_ref.at[k, c], local_sems.at[k * parts + c]
        )
        for k in range(slots)
        for c in range(parts)
    ]
    held = pltpu.make_async_copy(table_from, table_ref, local_sems.at[slots * parts + 1])
    for copy in [own, *fetches, held]:
        copy.start()
    around = Around(send_sems, recv_sems)
    around.meet()

    def meanwhile():
        grad_ref[...] = jnp.zeros_like(grad_ref)
        order = order_columns(size)
        for k in range(slots):
            for c in range(parts):
                fetches[k * parts + c].wait()
            put_in_order(raw_ref.at[k], measured_ref.at[k], order)
        for copy in [own, held]:
            copy.wait()

    rests = [pad(around, field_ref, padded_refs[0], relay_ref.at[0], meanwhile)]
    for k in range(ITERS):
        last = k == ITERS - 1
        add_terms(
            positions_ref, padded_refs[k], probes_ref, measured_ref, table_ref, grad_ref.at[k]
        )
        target = out_ref if last else padded_refs[k + 1]
        scratch = [ref.at[k] for ref in (mid_ref, side_ref, band_ref)]
        rests.append(step(last, around, grad_ref.at[k], padded_refs[k], target, *scratch, relay_ref.at[k + 1]))
    for rest in rests:
        rest()


def on_device(object_field, probe, positions, counts, intensity):
    planes, high, wide = object_field.shape
    slots, size, _ = intensity.shape[2:]
    table = jnp.asarray(tables(size))
    tall, broad = high + 2 * MARGIN, wide + 2 * MARGIN
    assert tall == broad == 2 * size
    copies = 64 * (ITERS + 1)
    floats = [
        *[(planes, tall, broad)] * ITERS,
        (ITERS, planes, tall, broad),
        (slots, size, size),
    ]
    blocks = [
        (ITERS, planes, tall, wide),
        (ITERS, 2, planes, tall, MARGIN),
        (ITERS, planes, tall, wide),
        (ITERS + 1, BLOCKS // 2, planes, MARGIN, wide),
    ]
    positions = positions[0, 0].T
    probes = pl.pallas_call(
        turn_kernel,
        out_shape=jax.ShapeDtypeStruct((slots, *probe.shape), jnp.float32),
        in_specs=[pl.BlockSpec(memory_space=pltpu.SMEM)] * 2 + [pl.BlockSpec(memory_space=pltpu.VMEM)],
        out_specs=pl.BlockSpec(memory_space=pltpu.VMEM),
        scratch_shapes=[pltpu.VMEM((planes, 2 * size, size), jnp.float32)],
        compiler_params=pltpu.CompilerParams(vmem_limit_bytes=12 * 1024 * 1024),
        name="turn",
    )(positions, counts, probe)
    held = [pltpu.with_memory_space_constraint(array, pltpu.HBM) for array in (object_field, intensity, table)]
    return pl.pallas_call(
        whole_kernel,
        out_shape=jax.ShapeDtypeStruct(object_field.shape, jnp.float32),
        in_specs=[pl.BlockSpec(memory_space=pltpu.SMEM)]
        + [pl.BlockSpec(memory_space=pltpu.HBM)] * 2
        + [pl.BlockSpec(memory_space=pltpu.VMEM), pl.BlockSpec(memory_space=pltpu.HBM)],
        out_specs=pl.BlockSpec(memory_space=pltpu.VMEM),
        scratch_shapes=[pltpu.VMEM(shape, jnp.float32) for shape in floats]
        + [
            pltpu.VMEM((slots, size // LANES, size, LANES), jnp.int32),
            pltpu.VMEM(table.shape, jnp.bfloat16),
        ]
        + [pltpu.VMEM(shape, jnp.float32) for shape in blocks]
        + [
            pltpu.SemaphoreType.DMA((copies,)),
            pltpu.SemaphoreType.DMA((copies,)),
            pltpu.SemaphoreType.DMA((slots * (size // LANES) + 3,)),
        ],
        compiler_params=pltpu.CompilerParams(
            collective_id=0, has_side_effects=True, vmem_limit_bytes=48 * 1024 * 1024
        ),
        name="whole",
    )(positions, *held[:2], probes, held[2])


def solution(mesh):
    placed = (
        P(None, "rows", "cols"),
        P(),
        P("rows", "cols", None, None),
        P("rows", "cols"),
        P("rows", "cols", None, None, None),
    )
    return jax.shard_map(
        on_device, mesh=mesh, in_specs=placed, out_specs=P(None, "rows", "cols"), check_vma=False
    )
```

```python
import functools
import itertools

import jax
import jax.numpy as jnp
import numpy as np
from jax import lax
from jax.experimental import pallas as pl
from jax.experimental.pallas import tpu as pltpu
from jax.sharding import PartitionSpec as P

MARGIN = 128
ITERS = 2
LANES = 128
ROWS = 8
PAIR = 2
BLOCKS = 4


step_rate = 0.02
photon_unit = 0.001


def tables(length):
    half = length // 2
    k = np.arange(half)[:, None]
    n = np.arange(half)[None, :]
    found = []
    for odd in (0, 1):
        angle = ((2 * k + odd) * n % length) * (2.0 * np.pi / length)
        c = np.cos(angle) / np.sqrt(length)
        s = np.sin(angle) / np.sqrt(length)
        full = np.block([[c, s], [-s, c]])
        found += [full, full.T]
    full = np.stack(found).astype(np.float32)
    high = full.astype(jnp.bfloat16)
    low = (full - high.astype(np.float32)).astype(jnp.bfloat16)
    return np.stack([high, low])


def dot(left, right):
    return lax.dot_general(left, right, (((1,), (0,)), ((), ())), preferred_element_type=jnp.float32)


def parted(value):
    high = value.astype(jnp.bfloat16)
    return high, (value - high.astype(jnp.float32)).astype(jnp.bfloat16)


def order_columns(length):
    half = length // 2
    here = lax.broadcasted_iota(jnp.int32, (length, length), 0)
    there = lax.broadcasted_iota(jnp.int32, (length, length), 1)
    wanted = jnp.where(there < half, 2 * there, 2 * there - length + 1)
    return jnp.where(here == wanted, 1.0, 0.0).astype(jnp.bfloat16)


def put_in_order(raw_ref, measured_ref, order):
    parts, size, _ = raw_ref.shape
    given = jnp.concatenate(
        [
            jnp.concatenate([raw_ref[c, pl.ds(odd, size // 2, stride=2)] for c in range(parts)], axis=1)
            for odd in (0, 1)
        ],
        axis=0,
    )

    def placed(value):
        return dot(value.astype(jnp.float32).astype(jnp.bfloat16), order)

    measured_ref[...] = (placed(given >> 4) * 16.0 + placed(given & 15)) * photon_unit


def from_left(table, which, value):
    high, low = value
    table = jnp.concatenate([table[0, which], table[1, which], table[0, which]], axis=1)
    return dot(table, jnp.concatenate([high, high, low], axis=0))


def from_right(table, which, value):
    high, low = value
    table = jnp.concatenate([table[0, which], table[1, which], table[0, which]], axis=0)
    return dot(jnp.concatenate([high, high, low], axis=1), table)


def turned(value, drop, shift):
    rows, columns = value.shape
    groups = pltpu.roll(value.reshape(rows // ROWS, ROWS, columns), drop, 1)
    before = jnp.concatenate([groups[-1:], groups[:-1]], axis=0)
    within = lax.broadcasted_iota(jnp.int32, (1, ROWS, columns), 1) >= drop
    value = jnp.where(within, groups, before).reshape(rows, columns)
    parts = [pltpu.roll(value[:, c : c + LANES], shift, 1) for c in range(0, columns, LANES)]
    within = lax.broadcasted_iota(jnp.int32, (rows, LANES), 1) >= shift
    return jnp.concatenate([jnp.where(within, a, b) for a, b in zip(parts, parts[-1:] + parts[:-1])], axis=1)


def slot_stages(slot, positions_ref, padded_ref, probes_ref, measured_ref, table_ref, terms):
    size = probes_ref.shape[2]
    half = size // 2
    below = lax.broadcasted_iota(jnp.int32, (size, size), 0) >= positions_ref[0, slot]
    beside = lax.broadcasted_iota(jnp.int32, (size, size), 1) >= positions_ref[1, slot]

    def folded(p):
        upper = jnp.where(beside, padded_ref[p, :size, :size], padded_ref[p, :size, size:])
        lower = jnp.where(beside, padded_ref[p, size:, :size], padded_ref[p, size:, size:])
        return jnp.where(below, upper, lower)

    probe_r = probes_ref[slot, 0]
    probe_i = probes_ref[slot, 1]
    patch_r, patch_i = folded(0), folded(1)
    exit_r = probe_r * patch_r - probe_i * patch_i
    exit_i = probe_r * patch_i + probe_i * patch_r
    upper = jnp.concatenate([exit_r[:half], exit_i[:half]], axis=0)
    lower = jnp.concatenate([exit_r[half:], exit_i[half:]], axis=0)
    even, odd = parted(upper + lower), parted(upper - lower)
    yield
    even, odd = from_left(table_ref, 0, even), from_left(table_ref, 2, odd)
    yield
    half_r = jnp.concatenate([even[:half], odd[:half]], axis=0)
    half_i = jnp.concatenate([even[half:], odd[half:]], axis=0)
    left = jnp.concatenate([half_r[:, :half], half_i[:, :half]], axis=1)
    right = jnp.concatenate([half_r[:, half:], half_i[:, half:]], axis=1)
    values = [parted(left + right), parted(left - right)]
    yield
    specs = [from_right(table_ref, 2 * odd + 1, value) for odd, value in enumerate(values)]
    yield
    values = []
    for odd, spec in enumerate(specs):
        spec_r, spec_i = spec[:, :half], spec[:, half:]
        misfit = spec_r * spec_r + spec_i * spec_i - measured_ref[slot, :, odd * half : (odd + 1) * half]
        values.append(parted(jnp.concatenate([misfit * spec_r, misfit * spec_i], axis=1)))
    yield
    backs = [from_right(table_ref, 2 * odd, value) for odd, value in enumerate(values)]
    yield
    left = backs[0] + backs[1]
    right = backs[0] - backs[1]
    half_r = jnp.concatenate([left[:, :half], right[:, :half]], axis=1)
    half_i = jnp.concatenate([left[:, half:], right[:, half:]], axis=1)
    even = parted(jnp.concatenate([half_r[:half], half_i[:half]], axis=0))
    odd = parted(jnp.concatenate([half_r[half:], half_i[half:]], axis=0))
    yield
    even, odd = from_left(table_ref, 1, even), from_left(table_ref, 3, odd)
    yield
    upper = even + odd
    lower = even - odd
    back_r = jnp.concatenate([upper[:half], lower[:half]], axis=0)
    back_i = jnp.concatenate([upper[half:], lower[half:]], axis=0)
    term_r = probe_r * back_r + probe_i * back_i
    term_i = probe_r * back_i - probe_i * back_r
    for term in (term_r, term_i):
        upper, lower = jnp.where(below, term, 0.0), jnp.where(below, 0.0, term)
        terms.append([jnp.where(beside, t, 0.0) if left else jnp.where(beside, 0.0, t) for t in (upper, lower) for left in (1, 0)])


def side_by_side(works):
    works = list(works)
    while works:
        works = [work for work in works if next(work, works) is not works]


def roll_probe(live, row, column, probe):
    rows, columns = probe.shape
    each = lax.broadcasted_iota(jnp.int32, probe.shape, 1)

    def picked(flag, first, second):
        return jnp.where(each < flag * columns, first, second)

    value = turned(probe, lax.rem(row, ROWS), lax.rem(column, LANES))
    step = LANES
    while step < columns:
        moved = jnp.concatenate([value[:, columns - step :], value[:, : columns - step]], axis=1)
        value = picked(lax.rem(lax.div(column, step), 2), moved, value)
        step *= 2
    step = ROWS
    while step < rows:
        moved = jnp.concatenate([value[rows - step :], value[: rows - step]], axis=0)
        value = picked(lax.rem(lax.div(row, step), 2), moved, value)
        step *= 2
    return picked(live, value, 0.0)


def add_terms(positions_ref, padded_ref, probes_ref, measured_ref, table_ref, grad_ref):
    planes = padded_ref.shape[0]
    slots, size, _ = measured_ref.shape

    def group(begin, width):
        terms = [[] for _ in range(width)]
        side_by_side(
            slot_stages(begin + k, positions_ref, padded_ref, probes_ref, measured_ref, table_ref, terms[k])
            for k in range(width)
        )
        for p in range(planes):
            for k, (r, c) in enumerate(itertools.product((0, size), (0, size))):
                grad_ref[p, r : r + size, c : c + size] += sum(term[p][k] for term in terms)

    @pl.loop(0, slots // PAIR)
    def _(step):
        group(step * PAIR, PAIR)

    for slot in range(slots // PAIR * PAIR, slots):
        group(slot, 1)


MESH = pl.DeviceIdType.MESH


class Around:
    def __init__(self, send_sems, recv_sems):
        self.send_sems, self.recv_sems = send_sems, recv_sems
        self.sends = self.recvs = 0
        self.here, self.device = {}, {}
        for axis in ("rows", "cols"):
            count = lax.axis_size(axis)
            me = lax.axis_index(axis)
            for d in (-2, -1, 1, 2):
                self.here[axis, d] = me + d >= 0 if d < 0 else me + d < count
                self.device[axis, d] = {axis: lax.rem(me + count + d, count)}
        count = lax.axis_size("rows")
        self.relays = count > 2 and count % 2 == 0
        odd = lax.rem(lax.axis_index("rows"), 2) == 1
        self.far = {1: odd, -1: no(odd)}

    def meet(self):
        barrier = pltpu.get_barrier_semaphore()
        sides = [("rows", -1), ("rows", 1), ("cols", -1), ("cols", 1)]
        if self.relays:
            sides += [("rows", -2), ("rows", 2)]
        for side in sides:

            @pl.when(self.here[side])
            def _():
                pl.semaphore_signal(barrier, inc=1, device_id=self.device[side], device_id_type=MESH)

        pl.semaphore_wait(barrier, sum(self.here[side].astype(jnp.int32) for side in sides))

    def new_recv(self):
        self.recvs += 1
        return self.recvs - 1

    def copy(self, side, source, target, recv=None):
        recv = self.new_recv() if recv is None else recv
        self.sends += 1
        return pltpu.make_async_remote_copy(
            src_ref=source,
            dst_ref=target,
            send_sem=self.send_sems.at[self.sends - 1],
            recv_sem=self.recv_sems.at[recv],
            device_id=self.device[side],
            device_id_type=MESH,
        )


class Side:
    def __init__(self, around, axis, d, source, target):
        self.here, self.back = around.here[axis, d], around.here[axis, -d]
        self.straight = around.copy((axis, d), source, target)

    def start(self):
        pl.when(self.here)(self.straight.start)

    def forward(self):
        pass

    def wait_recv(self):
        pl.when(self.back)(self.straight.wait_recv)

    def wait_left(self):
        pl.when(self.here)(self.straight.wait_send)

    def wait_forwarded(self):
        pass


class Hop:
    def __init__(self, around, d, source, target, relay):
        here, far = around.here["rows", d], around.far[d]
        self.back = around.here["rows", -d]
        recv = around.new_recv()
        self.straight = around.copy(("rows", d), source, target, recv)
        self.near = both(here, no(far))
        self.long = both(here, far)
        self.middle = both(around.here["rows", -2 * d], far)
        self.first = around.copy(("rows", 2 * d), source, relay)
        self.second = around.copy(("rows", -d), relay, target, recv)

    def start(self):
        pl.when(self.near)(self.straight.start)
        pl.when(self.long)(self.first.start)

    def forward(self):
        @pl.when(self.middle)
        def _():
            self.first.wait_recv()
            self.second.start()

    def wait_recv(self):
        pl.when(self.back)(self.straight.wait_recv)

    def wait_left(self):
        pl.when(self.near)(self.straight.wait_send)
        pl.when(self.long)(self.first.wait_send)

    def wait_forwarded(self):
        pl.when(self.middle)(self.second.wait_send)


def both(first, second):
    return jnp.logical_and(first, second)


def no(flag):
    return jnp.logical_not(flag)


def pad(around, field_ref, out_ref, relay_ref, meanwhile, afterwards):
    m = MARGIN
    planes, high, wide = field_ref.shape
    here = around.here
    part = m // 2
    row_from = {(-1, q): pl.ds(q * part, part) for q in (0, 1)} | {(1, q): pl.ds(high - m + q * part, part) for q in (0, 1)}
    row_land = {(1, q): pl.ds(q * part, part) for q in (0, 1)} | {(-1, q): pl.ds(m + high + q * part, part) for q in (0, 1)}
    col_cuts = {-1: (pl.ds(0, m), pl.ds(m + wide, m)), 1: (pl.ds(wide - m, m), pl.ds(0, m))}
    from_cuts = {-1: pl.ds(0, m), 1: pl.ds(m + high, m)}
    col_from = {-1: pl.ds(m, m), 1: pl.ds(wide, m)}
    rows, cols, corners = {}, {}, {}
    for d in (-1, 1):
        for q in (0, 1):
            source, target = field_ref.at[:, row_from[d, q]], out_ref.at[:, row_land[d, q], pl.ds(m, wide)]
            if around.relays and q == 0:
                rows[d, q] = Hop(around, d, source, target, relay_ref.at[0, :, pl.ds(0, part)])
            else:
                rows[d, q] = Side(around, "rows", d, source, target)
        cut, land = col_cuts[d]
        cols[d] = Side(around, "cols", d, field_ref.at[:, :, cut], out_ref.at[:, pl.ds(m, high), land])
        for v in (-1, 1):
            for q in (0, 1):
                lines = row_land[-v, q]
                corners[v, q, d] = around.copy(("cols", d), out_ref.at[:, lines, col_from[d]], out_ref.at[:, lines, land])
    for q in (0, 1):
        for d in (-1, 1):
            rows[d, q].start()
    for d in (-1, 1):
        cols[d].start()
    for v in (-1, 1):

        @pl.when(no(here["rows", v]))
        def _():
            out_ref[:, from_cuts[v], m : m + wide] = jnp.zeros((planes, m, wide), jnp.float32)

        for d in (-1, 1):
            land = col_cuts[-d][1]

            @pl.when(no(both(here["rows", v], here["cols", d])))
            def _():
                out_ref[:, from_cuts[v], land] = jnp.zeros((planes, m, m), jnp.float32)

    for d in (-1, 1):
        land = col_cuts[-d][1]

        @pl.when(no(here["cols", d]))
        def _():
            out_ref[:, m : m + high, land] = jnp.zeros((planes, high, m), jnp.float32)

    meanwhile()
    for d in (-1, 1):
        rows[d, 0].forward()
    afterwards()
    for far in (-1, 1):

        @pl.when(around.far[far])
        def _():
            for v, q in ((-far, 0), (-far, 1), (far, 1), (far, 0)):
                rows[-v, q].wait_recv()
                for d in (-1, 1):
                    pl.when(both(here["rows", v], here["cols", d]))(corners[v, q, d].start)

    for d in (-1, 1):
        cols[-d].wait_recv()
        for v in (-1, 1):
            for q in (0, 1):
                pl.when(both(here["rows", v], here["cols", d]))(corners[v, q, -d].wait_recv)
    def rest():
        for copy in [*rows.values(), *cols.values()]:
            copy.wait_left()
            copy.wait_forwarded()
        for v, q, d in corners:
            pl.when(both(here["rows", v], here["cols", d]))(corners[v, q, d].wait_send)

    return rest


def step(last, around, grad_ref, padded_ref, out_ref, mid_ref, side_ref, band_ref, relay_ref):
    m = MARGIN
    planes, extent, _ = grad_ref.shape
    wide = extent - 2 * m
    part = extent // 2 // BLOCKS
    outside = m // part
    here = around.here
    begin = {(h, q): q * part if h < 0 else extent - (q + 1) * part for h in (-1, 1) for q in range(BLOCKS)}
    lines = {key: pl.ds(start, part) for key, start in begin.items()}
    cut = {-1: pl.ds(0, m), 1: pl.ds(extent - m, m)}
    inner = {-1: pl.ds(m, m), 1: pl.ds(wide, m)}
    sent = range(outside if last else BLOCKS)
    relayed = len(sent) // 2
    sides, bands, edges = {}, {}, {}
    for q in range(BLOCKS):
        for h in (-1, 1):
            for d in (-1, 1):
                sides[h, q, d] = Side(
                    around, "cols", d, grad_ref.at[:, lines[h, q], cut[d]], side_ref.at[(d + 1) // 2, :, lines[h, q]]
                )
                if not last:
                    edges[h, q, d] = Side(
                        around, "cols", d, out_ref.at[:, lines[h, q], inner[d]], out_ref.at[:, lines[h, q], cut[-d]]
                    )
            if q not in sent:
                continue
            source, target = mid_ref.at[:, lines[h, q]], band_ref.at[:, lines[-h, BLOCKS - 1 - q]]
            if around.relays and q < relayed:
                bands[h, q] = Hop(around, h, source, target, relay_ref.at[q, :, pl.ds(0, part)])
            else:
                bands[h, q] = Side(around, "rows", h, source, target)
    for side in sides.values():
        side.start()
    if not last:
        for d in (-1, 1):

            @pl.when(no(here["cols", d]))
            def _():
                out_ref[:, :, cut[d]] = jnp.zeros((planes, extent, m), jnp.float32)

    def gather(h, q):
        mid_ref[:, lines[h, q]] = grad_ref[:, lines[h, q], m : m + wide]
        for d in (-1, 1):
            target = pl.ds(0, m) if d < 0 else pl.ds(wide - m, m)

            @pl.when(here["cols", d])
            def _():
                sides[h, q, -d].straight.wait_recv()
                mid_ref[:, lines[h, q], target] += side_ref[(1 - d) // 2, :, lines[h, q]]

    def finish(h, q):
        rows = lines[h, q]
        place = (slice(None), pl.ds(rows.start - m, part)) if last else (slice(None), rows, slice(m, m + wide))

        @pl.when(here["rows", h])
        def _():
            bands[-h, BLOCKS - 1 - q].straight.wait_recv()
            total = mid_ref[:, rows] + band_ref[:, rows]
            out_ref[place] = padded_ref[:, rows, m : m + wide] - step_rate * total

        @pl.when(no(here["rows", h]))
        def _():
            if q < outside:
                out_ref[place] = jnp.zeros((planes, part, wide), jnp.float32)
            else:
                out_ref[place] = padded_ref[:, rows, m : m + wide] - step_rate * mid_ref[:, rows]

        if not last:
            for d in (-1, 1):
                edges[h, q, d].start()

    def by_parity(work):
        for far in (-1, 1):
            pl.when(around.far[far])(functools.partial(work, far))

    for q in range(BLOCKS):
        for h in (-1, 1):
            gather(h, q)
            if q in sent:
                bands[h, q].start()
    for band in bands.values():
        band.forward()

    def finish_all(far):
        near = [(-far, q) for q in sent]
        order = near[:relayed]
        for q in sent[relayed:]:
            order += [near[q], (far, q)]
        for h, q in order + [(far, q) for q in sent[:relayed]]:
            finish(h, BLOCKS - 1 - q)

    by_parity(finish_all)
    for edge in edges.values():
        edge.wait_recv()
    def rest():
        for copy in [*bands.values(), *edges.values(), *sides.values()]:
            copy.wait_left()
            copy.wait_forwarded()

    return rest


def whole_kernel(
    positions_ref,
    counts_ref,
    field_ref,
    intensity_ref,
    probe_from,
    table_from,
    out_ref,
    *refs,
):
    padded_refs, refs = refs[:ITERS], refs[ITERS:]
    work(
        positions_ref, counts_ref, field_ref, intensity_ref, probe_from, table_from, out_ref, padded_refs, *refs
    )


def work(
    positions_ref,
    counts_ref,
    field_ref,
    intensity_ref,
    probe_from,
    table_from,
    out_ref,
    padded_refs,
    grad_ref,
    measured_ref,
    probes_ref,
    raw_ref,
    probe_ref,
    table_ref,
    mid_ref,
    side_ref,
    band_ref,
    relay_ref,
    send_sems,
    recv_sems,
    local_sems,
):
    m = MARGIN
    planes, high, wide = field_ref.shape
    slots, size, _ = measured_ref.shape
    parts = size // LANES
    own = pltpu.make_async_copy(
        field_ref, padded_refs[0].at[:, pl.ds(m, high), pl.ds(m, wide)], local_sems.at[slots * parts]
    )
    fetches = [
        pltpu.make_async_copy(
            intensity_ref.at[0, 0, k, :, pl.ds(c * LANES, LANES)], raw_ref.at[k, c], local_sems.at[k * parts + c]
        )
        for k in range(slots)
        for c in range(parts)
    ]
    held = [
        pltpu.make_async_copy(source, target, local_sems.at[slots * parts + 1 + k])
        for k, (source, target) in enumerate([(probe_from, probe_ref), (table_from, table_ref)])
    ]
    for copy in [own, *fetches, *held]:
        copy.start()
    around = Around(send_sems, recv_sems)
    around.meet()

    def meanwhile():
        grad_ref[...] = jnp.zeros_like(grad_ref)
        order = order_columns(size)
        for k in range(slots):
            for c in range(parts):
                fetches[k * parts + c].wait()
            put_in_order(raw_ref.at[k], measured_ref.at[k], order)

    def afterwards():
        for copy in [own, *held]:
            copy.wait()

        @pl.loop(0, slots)
        def _(slot):
            live = counts_ref[0, 0] - slot
            for p in range(planes):
                probes_ref[slot, p] = roll_probe(live, positions_ref[0, slot], positions_ref[1, slot], probe_ref[p])

    rests = [pad(around, field_ref, padded_refs[0], relay_ref.at[0], meanwhile, afterwards)]
    for k in range(ITERS):
        last = k == ITERS - 1
        add_terms(
            positions_ref, padded_refs[k], probes_ref, measured_ref, table_ref, grad_ref.at[k]
        )
        target = out_ref if last else padded_refs[k + 1]
        scratch = [ref.at[k] for ref in (mid_ref, side_ref, band_ref)]
        rests.append(step(last, around, grad_ref.at[k], padded_refs[k], target, *scratch, relay_ref.at[k + 1]))
    for rest in rests:
        rest()


def on_device(object_field, probe, positions, counts, intensity):
    planes, high, wide = object_field.shape
    slots, size, _ = intensity.shape[2:]
    table = jnp.asarray(tables(size))
    tall, broad = high + 2 * MARGIN, wide + 2 * MARGIN
    assert tall == broad == 2 * size
    copies = 64 * (ITERS + 1)
    floats = [
        *[(planes, tall, broad)] * ITERS,
        (ITERS, planes, tall, broad),
        (slots, size, size),
        (slots, planes, size, size),
    ]
    blocks = [
        (ITERS, planes, tall, wide),
        (ITERS, 2, planes, tall, MARGIN),
        (ITERS, planes, tall, wide),
        (ITERS + 1, BLOCKS // 2, planes, MARGIN, wide),
    ]
    held = [pltpu.with_memory_space_constraint(array, pltpu.HBM) for array in (object_field, intensity, probe, table)]
    return pl.pallas_call(
        whole_kernel,
        out_shape=jax.ShapeDtypeStruct(object_field.shape, jnp.float32),
        in_specs=[pl.BlockSpec(memory_space=pltpu.SMEM)] * 2 + [pl.BlockSpec(memory_space=pltpu.HBM)] * len(held),
        out_specs=pl.BlockSpec(memory_space=pltpu.VMEM),
        scratch_shapes=[pltpu.VMEM(shape, jnp.float32) for shape in floats]
        + [
            pltpu.VMEM((slots, size // LANES, size, LANES), jnp.int32),
            pltpu.VMEM(probe.shape, jnp.float32),
            pltpu.VMEM(table.shape, jnp.bfloat16),
        ]
        + [pltpu.VMEM(shape, jnp.float32) for shape in blocks]
        + [
            pltpu.SemaphoreType.DMA((copies,)),
            pltpu.SemaphoreType.DMA((copies,)),
            pltpu.SemaphoreType.DMA((slots * (size // LANES) + 3,)),
        ],
        compiler_params=pltpu.CompilerParams(
            collective_id=0, has_side_effects=True, vmem_limit_bytes=48 * 1024 * 1024
        ),
        name="whole",
    )(positions[0, 0].T, counts, *held)


def solution(mesh):
    placed = (
        P(None, "rows", "cols"),
        P(),
        P("rows", "cols", None, None),
        P("rows", "cols"),
        P("rows", "cols", None, None, None),
    )
    return jax.shard_map(
        on_device, mesh=mesh, in_specs=placed, out_specs=P(None, "rows", "cols"), check_vma=False
    )
```

```python
import functools
import itertools

import jax
import jax.numpy as jnp
import numpy as np
from jax import lax
from jax.experimental import pallas as pl
from jax.experimental.pallas import tpu as pltpu
from jax.sharding import PartitionSpec as P

MARGIN = 128
ITERS = 2
LANES = 128
ROWS = 8
PAIR = 2
BLOCKS = 2


step_rate = 0.02
photon_unit = 0.001


def tables(length):
    half = length // 2
    k = np.arange(half)[:, None]
    n = np.arange(half)[None, :]
    found = []
    for odd in (0, 1):
        angle = ((2 * k + odd) * n % length) * (2.0 * np.pi / length)
        c = np.cos(angle) / np.sqrt(length)
        s = np.sin(angle) / np.sqrt(length)
        full = np.block([[c, s], [-s, c]])
        found += [full, full.T]
    full = np.stack(found).astype(np.float32)
    high = full.astype(jnp.bfloat16)
    low = (full - high.astype(np.float32)).astype(jnp.bfloat16)
    return np.stack([high, low])


def dot(left, right):
    return lax.dot_general(left, right, (((1,), (0,)), ((), ())), preferred_element_type=jnp.float32)


def parted(value):
    high = value.astype(jnp.bfloat16)
    return high, (value - high.astype(jnp.float32)).astype(jnp.bfloat16)


def order_columns(length):
    half = length // 2
    here = lax.broadcasted_iota(jnp.int32, (length, length), 0)
    there = lax.broadcasted_iota(jnp.int32, (length, length), 1)
    wanted = jnp.where(there < half, 2 * there, 2 * there - length + 1)
    return jnp.where(here == wanted, 1.0, 0.0).astype(jnp.bfloat16)


def put_in_order(raw_ref, measured_ref, order):
    parts, size, _ = raw_ref.shape
    given = jnp.concatenate(
        [
            jnp.concatenate([raw_ref[c, pl.ds(odd, size // 2, stride=2)] for c in range(parts)], axis=1)
            for odd in (0, 1)
        ],
        axis=0,
    )

    def placed(value):
        return dot(value.astype(jnp.float32).astype(jnp.bfloat16), order)

    measured_ref[...] = (placed(given >> 4) * 16.0 + placed(given & 15)) * photon_unit


def from_left(table, which, value):
    high, low = value
    table = jnp.concatenate([table[0, which], table[1, which], table[0, which]], axis=1)
    return dot(table, jnp.concatenate([high, high, low], axis=0))


def from_right(table, which, value):
    high, low = value
    table = jnp.concatenate([table[0, which], table[1, which], table[0, which]], axis=0)
    return dot(jnp.concatenate([high, high, low], axis=1), table)


def turned(value, drop, shift):
    rows, columns = value.shape
    groups = pltpu.roll(value.reshape(rows // ROWS, ROWS, columns), drop, 1)
    before = jnp.concatenate([groups[-1:], groups[:-1]], axis=0)
    within = lax.broadcasted_iota(jnp.int32, (1, ROWS, columns), 1) >= drop
    value = jnp.where(within, groups, before).reshape(rows, columns)
    parts = [pltpu.roll(value[:, c : c + LANES], shift, 1) for c in range(0, columns, LANES)]
    within = lax.broadcasted_iota(jnp.int32, (rows, LANES), 1) >= shift
    return jnp.concatenate([jnp.where(within, a, b) for a, b in zip(parts, parts[-1:] + parts[:-1])], axis=1)


def slot_stages(slot, positions_ref, padded_ref, probes_ref, measured_ref, table_ref, terms):
    size = probes_ref.shape[2]
    half = size // 2
    below = lax.broadcasted_iota(jnp.int32, (size, size), 0) >= positions_ref[0, slot]
    beside = lax.broadcasted_iota(jnp.int32, (size, size), 1) >= positions_ref[1, slot]

    def folded(p):
        upper = jnp.where(beside, padded_ref[p, :size, :size], padded_ref[p, :size, size:])
        lower = jnp.where(beside, padded_ref[p, size:, :size], padded_ref[p, size:, size:])
        return jnp.where(below, upper, lower)

    probe_r = probes_ref[slot, 0]
    probe_i = probes_ref[slot, 1]
    patch_r, patch_i = folded(0), folded(1)
    exit_r = probe_r * patch_r - probe_i * patch_i
    exit_i = probe_r * patch_i + probe_i * patch_r
    upper = jnp.concatenate([exit_r[:half], exit_i[:half]], axis=0)
    lower = jnp.concatenate([exit_r[half:], exit_i[half:]], axis=0)
    even, odd = parted(upper + lower), parted(upper - lower)
    yield
    even, odd = from_left(table_ref, 0, even), from_left(table_ref, 2, odd)
    yield
    half_r = jnp.concatenate([even[:half], odd[:half]], axis=0)
    half_i = jnp.concatenate([even[half:], odd[half:]], axis=0)
    left = jnp.concatenate([half_r[:, :half], half_i[:, :half]], axis=1)
    right = jnp.concatenate([half_r[:, half:], half_i[:, half:]], axis=1)
    values = [parted(left + right), parted(left - right)]
    yield
    specs = [from_right(table_ref, 2 * odd + 1, value) for odd, value in enumerate(values)]
    yield
    values = []
    for odd, spec in enumerate(specs):
        spec_r, spec_i = spec[:, :half], spec[:, half:]
        misfit = spec_r * spec_r + spec_i * spec_i - measured_ref[slot, :, odd * half : (odd + 1) * half]
        values.append(parted(jnp.concatenate([misfit * spec_r, misfit * spec_i], axis=1)))
    yield
    backs = [from_right(table_ref, 2 * odd, value) for odd, value in enumerate(values)]
    yield
    left = backs[0] + backs[1]
    right = backs[0] - backs[1]
    half_r = jnp.concatenate([left[:, :half], right[:, :half]], axis=1)
    half_i = jnp.concatenate([left[:, half:], right[:, half:]], axis=1)
    even = parted(jnp.concatenate([half_r[:half], half_i[:half]], axis=0))
    odd = parted(jnp.concatenate([half_r[half:], half_i[half:]], axis=0))
    yield
    even, odd = from_left(table_ref, 1, even), from_left(table_ref, 3, odd)
    yield
    upper = even + odd
    lower = even - odd
    back_r = jnp.concatenate([upper[:half], lower[:half]], axis=0)
    back_i = jnp.concatenate([upper[half:], lower[half:]], axis=0)
    term_r = probe_r * back_r + probe_i * back_i
    term_i = probe_r * back_i - probe_i * back_r
    for term in (term_r, term_i):
        upper, lower = jnp.where(below, term, 0.0), jnp.where(below, 0.0, term)
        terms.append([jnp.where(beside, t, 0.0) if left else jnp.where(beside, 0.0, t) for t in (upper, lower) for left in (1, 0)])


def side_by_side(works):
    works = list(works)
    while works:
        works = [work for work in works if next(work, works) is not works]


def roll_probe(live, row, column, probe):
    rows, columns = probe.shape
    each = lax.broadcasted_iota(jnp.int32, probe.shape, 1)

    def picked(flag, first, second):
        return jnp.where(each < flag * columns, first, second)

    value = turned(probe, lax.rem(row, ROWS), lax.rem(column, LANES))
    step = LANES
    while step < columns:
        moved = jnp.concatenate([value[:, columns - step :], value[:, : columns - step]], axis=1)
        value = picked(lax.rem(lax.div(column, step), 2), moved, value)
        step *= 2
    step = ROWS
    while step < rows:
        moved = jnp.concatenate([value[rows - step :], value[: rows - step]], axis=0)
        value = picked(lax.rem(lax.div(row, step), 2), moved, value)
        step *= 2
    return picked(live, value, 0.0)


def add_terms(positions_ref, padded_ref, probes_ref, measured_ref, table_ref, grad_ref):
    planes = padded_ref.shape[0]
    slots, size, _ = measured_ref.shape

    def group(begin, width):
        terms = [[] for _ in range(width)]
        side_by_side(
            slot_stages(begin + k, positions_ref, padded_ref, probes_ref, measured_ref, table_ref, terms[k])
            for k in range(width)
        )
        for p in range(planes):
            for k, (r, c) in enumerate(itertools.product((0, size), (0, size))):
                grad_ref[p, r : r + size, c : c + size] += sum(term[p][k] for term in terms)

    @pl.loop(0, slots // PAIR)
    def _(step):
        group(step * PAIR, PAIR)

    for slot in range(slots // PAIR * PAIR, slots):
        group(slot, 1)


MESH = pl.DeviceIdType.MESH


class Around:
    def __init__(self, send_sems, recv_sems):
        self.send_sems, self.recv_sems = send_sems, recv_sems
        self.sends = self.recvs = 0
        self.here, self.device = {}, {}
        for axis in ("rows", "cols"):
            count = lax.axis_size(axis)
            me = lax.axis_index(axis)
            for d in (-2, -1, 1, 2):
                self.here[axis, d] = me + d >= 0 if d < 0 else me + d < count
                self.device[axis, d] = {axis: lax.rem(me + count + d, count)}
        count = lax.axis_size("rows")
        self.relays = count > 2 and count % 2 == 0
        odd = lax.rem(lax.axis_index("rows"), 2) == 1
        self.far = {1: odd, -1: no(odd)}
        even = lax.rem(lax.axis_index("cols"), 2) == 0
        self.quick = {1: even, -1: no(even)}

    def meet(self):
        barrier = pltpu.get_barrier_semaphore()
        sides = [("rows", -1), ("rows", 1), ("cols", -1), ("cols", 1)]
        if self.relays:
            sides += [("rows", -2), ("rows", 2)]
        for side in sides:

            @pl.when(self.here[side])
            def _():
                pl.semaphore_signal(barrier, inc=1, device_id=self.device[side], device_id_type=MESH)

        pl.semaphore_wait(barrier, sum(self.here[side].astype(jnp.int32) for side in sides))

    def new_recv(self):
        self.recvs += 1
        return self.recvs - 1

    def copy(self, side, source, target, recv=None):
        recv = self.new_recv() if recv is None else recv
        self.sends += 1
        return pltpu.make_async_remote_copy(
            src_ref=source,
            dst_ref=target,
            send_sem=self.send_sems.at[self.sends - 1],
            recv_sem=self.recv_sems.at[recv],
            device_id=self.device[side],
            device_id_type=MESH,
        )


class Side:
    def __init__(self, around, axis, d, source, target):
        self.here, self.back = around.here[axis, d], around.here[axis, -d]
        self.straight = around.copy((axis, d), source, target)

    def start(self):
        pl.when(self.here)(self.straight.start)

    def forward(self):
        pass

    def wait_recv(self):
        pl.when(self.back)(self.straight.wait_recv)

    def wait_left(self):
        pl.when(self.here)(self.straight.wait_send)

    def wait_forwarded(self):
        pass


class Hop:
    def __init__(self, around, d, c, source, target, relay):
        here = around.here["rows", d]
        by = both(around.far[d], around.quick[c]) if around.relays else False
        self.back = around.here["rows", -d]
        recv = around.new_recv()
        self.straight = around.copy(("rows", d), source, target, recv)
        self.near = both(here, no(by))
        self.long = both(here, by)
        self.middle = both(around.here["rows", -2 * d], by)
        self.first = around.copy(("rows", 2 * d), source, relay)
        self.second = around.copy(("rows", -d), relay, target, recv)

    def start(self):
        pl.when(self.near)(self.straight.start)
        pl.when(self.long)(self.first.start)

    def forward(self):
        @pl.when(self.middle)
        def _():
            self.first.wait_recv()
            self.second.start()

    def wait_recv(self):
        pl.when(self.back)(self.straight.wait_recv)

    def wait_left(self):
        pl.when(self.near)(self.straight.wait_send)
        pl.when(self.long)(self.first.wait_send)

    def wait_forwarded(self):
        pl.when(self.middle)(self.second.wait_send)


def both(first, second):
    return jnp.logical_and(first, second)


def no(flag):
    return jnp.logical_not(flag)


def pad(around, field_ref, out_ref, relay_ref, meanwhile, afterwards):
    m = MARGIN
    planes, high, wide = field_ref.shape
    here = around.here
    sides = (-1, 1)
    row_from = {-1: pl.ds(0, m), 1: pl.ds(high - m, m)}
    row_land = {1: pl.ds(0, m), -1: pl.ds(m + high, m)}
    half = {-1: pl.ds(0, m), 1: pl.ds(wide - m, m)}
    inner = {-1: pl.ds(m, m), 1: pl.ds(wide, m)}
    col_cuts = {-1: (pl.ds(0, m), pl.ds(m + wide, m)), 1: (pl.ds(wide - m, m), pl.ds(0, m))}
    from_cuts = {-1: pl.ds(0, m), 1: pl.ds(m + high, m)}
    rows, cols, corners = {}, {}, {}
    for d in sides:
        cut, land = col_cuts[d]
        cols[d] = Side(around, "cols", d, field_ref.at[:, :, cut], out_ref.at[:, pl.ds(m, high), land])
        for c in sides:
            source, target = field_ref.at[:, row_from[d], half[c]], out_ref.at[:, row_land[d], inner[c]]
            rows[d, c] = Hop(around, d, c, source, target, relay_ref.at[0, :, pl.ds(0, m), pl.ds(0, m)])
            corners[d, c] = around.copy(
                ("cols", c), out_ref.at[:, from_cuts[d], inner[c]], out_ref.at[:, from_cuts[d], col_cuts[c][1]]
            )

    def slow_first(work):
        for c in sides:
            pl.when(around.quick[-c])(functools.partial(work, (c, -c)))

    @slow_first
    def _(order):
        for c in order:
            for d in sides:
                rows[d, c].start()

    for d in sides:
        cols[d].start()
    for v in (-1, 1):

        @pl.when(no(here["rows", v]))
        def _():
            out_ref[:, from_cuts[v], m : m + wide] = jnp.zeros((planes, m, wide), jnp.float32)

        for d in (-1, 1):
            land = col_cuts[-d][1]

            @pl.when(no(both(here["rows", v], here["cols", d])))
            def _():
                out_ref[:, from_cuts[v], land] = jnp.zeros((planes, m, m), jnp.float32)

    for d in (-1, 1):
        land = col_cuts[-d][1]

        @pl.when(no(here["cols", d]))
        def _():
            out_ref[:, m : m + high, land] = jnp.zeros((planes, high, m), jnp.float32)

    meanwhile()
    for hop in rows.values():
        hop.forward()
    afterwards()

    def receive(far, order):
        for c in order:
            for v in (-far, far):
                rows[-v, c].wait_recv()
                pl.when(both(here["rows", v], here["cols", c]))(corners[v, c].start)

    for far in sides:
        pl.when(around.far[far])(lambda far=far: slow_first(functools.partial(receive, far)))
    for d in sides:
        cols[-d].wait_recv()
        for v in sides:
            pl.when(both(here["rows", v], here["cols", d]))(corners[v, -d].wait_recv)

    def rest():
        for copy in [*rows.values(), *cols.values()]:
            copy.wait_left()
            copy.wait_forwarded()
        for v, c in corners:
            pl.when(both(here["rows", v], here["cols", c]))(corners[v, c].wait_send)

    return rest


def step(last, around, grad_ref, padded_ref, out_ref, mid_ref, side_ref, band_ref, relay_ref):
    m = MARGIN
    planes, extent, _ = grad_ref.shape
    wide = extent - 2 * m
    part = extent // 2 // BLOCKS
    outside = m // part
    here = around.here
    begin = {(h, q): q * part if h < 0 else extent - (q + 1) * part for q in range(BLOCKS) for h in (-1, 1)}
    lines = {key: pl.ds(start, part) for key, start in begin.items()}
    cut = {-1: pl.ds(0, m), 1: pl.ds(extent - m, m)}
    inner = {-1: pl.ds(m, m), 1: pl.ds(wide, m)}
    half = {-1: pl.ds(0, m), 1: pl.ds(wide - m, m)}
    sent = range(outside if last else BLOCKS)
    sides, bands, edges = {}, {}, {}
    for h, q in lines:
        for d in (-1, 1):
            rows = lines[h, q]
            sides[h, q, d] = Side(around, "cols", d, grad_ref.at[:, rows, cut[d]], side_ref.at[(d + 1) // 2, :, rows])
            if not last:
                edges[h, q, d] = Side(around, "cols", d, out_ref.at[:, rows, inner[d]], out_ref.at[:, rows, cut[-d]])
            if q in sent:
                source, target = mid_ref.at[:, rows, half[d]], band_ref.at[:, lines[-h, BLOCKS - 1 - q], half[d]]
                relay = relay_ref.at[q, :, pl.ds(0, part), pl.ds(0, m)]
                bands[h, q, d] = Hop(around, h, d, source, target, relay)
    for side in sides.values():
        side.start()
    if not last:
        for d in (-1, 1):

            @pl.when(no(here["cols", d]))
            def _():
                out_ref[:, :, cut[d]] = jnp.zeros((planes, extent, m), jnp.float32)

    def gather(h, q, d):
        rows = lines[h, q]
        mid_ref[:, rows, half[d]] = grad_ref[:, rows, inner[d]]

        @pl.when(here["cols", d])
        def _():
            sides[h, q, -d].straight.wait_recv()
            mid_ref[:, rows, half[d]] += side_ref[(1 - d) // 2, :, rows]

    def finish(h, q, d):
        rows = lines[h, q]
        place = (slice(None), pl.ds(rows.start - m, part), half[d]) if last else (slice(None), rows, inner[d])

        @pl.when(here["rows", h])
        def _():
            bands[-h, BLOCKS - 1 - q, d].straight.wait_recv()
            total = mid_ref[:, rows, half[d]] + band_ref[:, rows, half[d]]
            out_ref[place] = padded_ref[:, rows, inner[d]] - step_rate * total

        @pl.when(no(here["rows", h]))
        def _():
            if q < outside:
                out_ref[place] = jnp.zeros((planes, part, m), jnp.float32)
            else:
                out_ref[place] = padded_ref[:, rows, inner[d]] - step_rate * mid_ref[:, rows, half[d]]

        if not last:
            edges[h, q, d].start()

    def begin_all(quick):
        for d in (quick, -quick):
            for q in range(BLOCKS):
                for h in (-1, 1):
                    gather(h, q, d)
                    if q in sent:
                        bands[h, q, d].start()

    def finish_all(far, quick):
        order = [(-far, q, quick) for q in sent]
        for q in sent:
            order += [(far, q, -quick), (-far, q, -quick)]
        for h, q, d in order + [(far, q, quick) for q in sent]:
            finish(h, BLOCKS - 1 - q, d)

    for quick in (-1, 1):
        pl.when(around.quick[quick])(functools.partial(begin_all, quick))
    for band in bands.values():
        band.forward()
    for far in (-1, 1):
        for quick in (-1, 1):
            pl.when(both(around.far[far], around.quick[quick]))(functools.partial(finish_all, far, quick))
    for edge in edges.values():
        edge.wait_recv()
    def rest():
        for copy in [*bands.values(), *edges.values(), *sides.values()]:
            copy.wait_left()
            copy.wait_forwarded()

    return rest


def whole_kernel(
    positions_ref,
    counts_ref,
    field_ref,
    intensity_ref,
    probe_from,
    table_from,
    out_ref,
    *refs,
):
    padded_refs, refs = refs[:ITERS], refs[ITERS:]
    work(
        positions_ref, counts_ref, field_ref, intensity_ref, probe_from, table_from, out_ref, padded_refs, *refs
    )


def work(
    positions_ref,
    counts_ref,
    field_ref,
    intensity_ref,
    probe_from,
    table_from,
    out_ref,
    padded_refs,
    grad_ref,
    measured_ref,
    probes_ref,
    raw_ref,
    probe_ref,
    table_ref,
    mid_ref,
    side_ref,
    band_ref,
    relay_ref,
    send_sems,
    recv_sems,
    local_sems,
):
    m = MARGIN
    planes, high, wide = field_ref.shape
    slots, size, _ = measured_ref.shape
    parts = size // LANES
    own = pltpu.make_async_copy(
        field_ref, padded_refs[0].at[:, pl.ds(m, high), pl.ds(m, wide)], local_sems.at[slots * parts]
    )
    fetches = [
        pltpu.make_async_copy(
            intensity_ref.at[0, 0, k, :, pl.ds(c * LANES, LANES)], raw_ref.at[k, c], local_sems.at[k * parts + c]
        )
        for k in range(slots)
        for c in range(parts)
    ]
    held = [
        pltpu.make_async_copy(source, target, local_sems.at[slots * parts + 1 + k])
        for k, (source, target) in enumerate([(probe_from, probe_ref), (table_from, table_ref)])
    ]
    for copy in [own, *fetches, *held]:
        copy.start()
    around = Around(send_sems, recv_sems)
    around.meet()

    def meanwhile():
        grad_ref[...] = jnp.zeros_like(grad_ref)
        order = order_columns(size)
        for k in range(slots):
            for c in range(parts):
                fetches[k * parts + c].wait()
            put_in_order(raw_ref.at[k], measured_ref.at[k], order)

    def afterwards():
        for copy in [own, *held]:
            copy.wait()

        @pl.loop(0, slots)
        def _(slot):
            live = counts_ref[0, 0] - slot
            for p in range(planes):
                probes_ref[slot, p] = roll_probe(live, positions_ref[0, slot], positions_ref[1, slot], probe_ref[p])

    rests = [pad(around, field_ref, padded_refs[0], relay_ref.at[0], meanwhile, afterwards)]
    for k in range(ITERS):
        last = k == ITERS - 1
        add_terms(
            positions_ref, padded_refs[k], probes_ref, measured_ref, table_ref, grad_ref.at[k]
        )
        target = out_ref if last else padded_refs[k + 1]
        scratch = [ref.at[k] for ref in (mid_ref, side_ref, band_ref)]
        rests.append(step(last, around, grad_ref.at[k], padded_refs[k], target, *scratch, relay_ref.at[k + 1]))
    for rest in rests:
        rest()


def on_device(object_field, probe, positions, counts, intensity):
    planes, high, wide = object_field.shape
    slots, size, _ = intensity.shape[2:]
    table = jnp.asarray(tables(size))
    tall, broad = high + 2 * MARGIN, wide + 2 * MARGIN
    assert tall == broad == 2 * size and wide == 2 * MARGIN
    copies = 64 * (ITERS + 1)
    floats = [
        *[(planes, tall, broad)] * ITERS,
        (ITERS, planes, tall, broad),
        (slots, size, size),
        (slots, planes, size, size),
    ]
    blocks = [
        (ITERS, planes, tall, wide),
        (ITERS, 2, planes, tall, MARGIN),
        (ITERS, planes, tall, wide),
        (ITERS + 1, BLOCKS, planes, MARGIN, MARGIN),
    ]
    held = [pltpu.with_memory_space_constraint(array, pltpu.HBM) for array in (object_field, intensity, probe, table)]
    return pl.pallas_call(
        whole_kernel,
        out_shape=jax.ShapeDtypeStruct(object_field.shape, jnp.float32),
        in_specs=[pl.BlockSpec(memory_space=pltpu.SMEM)] * 2 + [pl.BlockSpec(memory_space=pltpu.HBM)] * len(held),
        out_specs=pl.BlockSpec(memory_space=pltpu.VMEM),
        scratch_shapes=[pltpu.VMEM(shape, jnp.float32) for shape in floats]
        + [
            pltpu.VMEM((slots, size // LANES, size, LANES), jnp.int32),
            pltpu.VMEM(probe.shape, jnp.float32),
            pltpu.VMEM(table.shape, jnp.bfloat16),
        ]
        + [pltpu.VMEM(shape, jnp.float32) for shape in blocks]
        + [
            pltpu.SemaphoreType.DMA((copies,)),
            pltpu.SemaphoreType.DMA((copies,)),
            pltpu.SemaphoreType.DMA((slots * (size // LANES) + 3,)),
        ],
        compiler_params=pltpu.CompilerParams(
            collective_id=0, has_side_effects=True, vmem_limit_bytes=48 * 1024 * 1024
        ),
        name="whole",
    )(positions[0, 0].T, counts, *held)


def solution(mesh):
    placed = (
        P(None, "rows", "cols"),
        P(),
        P("rows", "cols", None, None),
        P("rows", "cols"),
        P("rows", "cols", None, None, None),
    )
    return jax.shard_map(
        on_device, mesh=mesh, in_specs=placed, out_specs=P(None, "rows", "cols"), check_vma=False
    )
```

```python
import functools
import itertools

import jax
import jax.numpy as jnp
import numpy as np
from jax import lax
from jax.experimental import pallas as pl
from jax.experimental.pallas import tpu as pltpu
from jax.sharding import PartitionSpec as P

MARGIN = 128
ITERS = 2
LANES = 128
ROWS = 8
PAIR = 2
BLOCKS = 2


step_rate = 0.02
photon_unit = 0.001


def tables(length):
    half = length // 2
    k = np.arange(half)[:, None]
    n = np.arange(half)[None, :]
    found = []
    for odd in (0, 1):
        angle = ((2 * k + odd) * n % length) * (2.0 * np.pi / length)
        c = np.cos(angle) / np.sqrt(length)
        s = np.sin(angle) / np.sqrt(length)
        full = np.block([[c, s], [-s, c]])
        found += [full, full.T]
    full = np.stack(found).astype(np.float32)
    high = full.astype(jnp.bfloat16)
    low = (full - high.astype(np.float32)).astype(jnp.bfloat16)
    return np.stack([high, low])


def dot(left, right):
    return lax.dot_general(left, right, (((1,), (0,)), ((), ())), preferred_element_type=jnp.float32)


def parted(value):
    high = value.astype(jnp.bfloat16)
    return high, (value - high.astype(jnp.float32)).astype(jnp.bfloat16)


def order_columns(length):
    half = length // 2
    here = lax.broadcasted_iota(jnp.int32, (length, length), 0)
    there = lax.broadcasted_iota(jnp.int32, (length, length), 1)
    wanted = jnp.where(there < half, 2 * there, 2 * there - length + 1)
    return jnp.where(here == wanted, 1.0, 0.0).astype(jnp.bfloat16)


def put_in_order(raw_ref, measured_ref, order):
    parts, size, _ = raw_ref.shape
    given = jnp.concatenate(
        [
            jnp.concatenate([raw_ref[c, pl.ds(odd, size // 2, stride=2)] for c in range(parts)], axis=1)
            for odd in (0, 1)
        ],
        axis=0,
    )

    def placed(value):
        return dot(value.astype(jnp.float32).astype(jnp.bfloat16), order)

    measured_ref[...] = (placed(given >> 4) * 16.0 + placed(given & 15)) * photon_unit


def from_left(table, which, value):
    high, low = value
    table = jnp.concatenate([table[0, which], table[1, which], table[0, which]], axis=1)
    return dot(table, jnp.concatenate([high, high, low], axis=0))


def from_right(table, which, value):
    high, low = value
    table = jnp.concatenate([table[0, which], table[1, which], table[0, which]], axis=0)
    return dot(jnp.concatenate([high, high, low], axis=1), table)


def turned(value, drop, shift):
    rows, columns = value.shape
    groups = pltpu.roll(value.reshape(rows // ROWS, ROWS, columns), drop, 1)
    before = jnp.concatenate([groups[-1:], groups[:-1]], axis=0)
    within = lax.broadcasted_iota(jnp.int32, (1, ROWS, columns), 1) >= drop
    value = jnp.where(within, groups, before).reshape(rows, columns)
    parts = [pltpu.roll(value[:, c : c + LANES], shift, 1) for c in range(0, columns, LANES)]
    within = lax.broadcasted_iota(jnp.int32, (rows, LANES), 1) >= shift
    return jnp.concatenate([jnp.where(within, a, b) for a, b in zip(parts, parts[-1:] + parts[:-1])], axis=1)


def slot_stages(slot, positions_ref, padded_ref, probes_ref, measured_ref, table_ref, terms):
    size = probes_ref.shape[2]
    half = size // 2
    below = lax.broadcasted_iota(jnp.int32, (size, size), 0) >= positions_ref[0, slot]
    beside = lax.broadcasted_iota(jnp.int32, (size, size), 1) >= positions_ref[1, slot]

    def folded(p):
        upper = jnp.where(beside, padded_ref[p, :size, :size], padded_ref[p, :size, size:])
        lower = jnp.where(beside, padded_ref[p, size:, :size], padded_ref[p, size:, size:])
        return jnp.where(below, upper, lower)

    probe_r = probes_ref[slot, 0]
    probe_i = probes_ref[slot, 1]
    patch_r, patch_i = folded(0), folded(1)
    exit_r = probe_r * patch_r - probe_i * patch_i
    exit_i = probe_r * patch_i + probe_i * patch_r
    upper = jnp.concatenate([exit_r[:half], exit_i[:half]], axis=0)
    lower = jnp.concatenate([exit_r[half:], exit_i[half:]], axis=0)
    even, odd = parted(upper + lower), parted(upper - lower)
    yield
    even, odd = from_left(table_ref, 0, even), from_left(table_ref, 2, odd)
    yield
    half_r = jnp.concatenate([even[:half], odd[:half]], axis=0)
    half_i = jnp.concatenate([even[half:], odd[half:]], axis=0)
    left = jnp.concatenate([half_r[:, :half], half_i[:, :half]], axis=1)
    right = jnp.concatenate([half_r[:, half:], half_i[:, half:]], axis=1)
    values = [parted(left + right), parted(left - right)]
    yield
    specs = [from_right(table_ref, 2 * odd + 1, value) for odd, value in enumerate(values)]
    yield
    values = []
    for odd, spec in enumerate(specs):
        spec_r, spec_i = spec[:, :half], spec[:, half:]
        misfit = spec_r * spec_r + spec_i * spec_i - measured_ref[slot, :, odd * half : (odd + 1) * half]
        values.append(parted(jnp.concatenate([misfit * spec_r, misfit * spec_i], axis=1)))
    yield
    backs = [from_right(table_ref, 2 * odd, value) for odd, value in enumerate(values)]
    yield
    left = backs[0] + backs[1]
    right = backs[0] - backs[1]
    half_r = jnp.concatenate([left[:, :half], right[:, :half]], axis=1)
    half_i = jnp.concatenate([left[:, half:], right[:, half:]], axis=1)
    even = parted(jnp.concatenate([half_r[:half], half_i[:half]], axis=0))
    odd = parted(jnp.concatenate([half_r[half:], half_i[half:]], axis=0))
    yield
    even, odd = from_left(table_ref, 1, even), from_left(table_ref, 3, odd)
    yield
    upper = even + odd
    lower = even - odd
    back_r = jnp.concatenate([upper[:half], lower[:half]], axis=0)
    back_i = jnp.concatenate([upper[half:], lower[half:]], axis=0)
    term_r = probe_r * back_r + probe_i * back_i
    term_i = probe_r * back_i - probe_i * back_r
    for term in (term_r, term_i):
        upper, lower = jnp.where(below, term, 0.0), jnp.where(below, 0.0, term)
        terms.append([jnp.where(beside, t, 0.0) if left else jnp.where(beside, 0.0, t) for t in (upper, lower) for left in (1, 0)])


def side_by_side(works):
    works = list(works)
    while works:
        works = [work for work in works if next(work, works) is not works]


def roll_probe(live, row, column, probe):
    rows, columns = probe.shape
    each = lax.broadcasted_iota(jnp.int32, probe.shape, 1)

    def picked(flag, first, second):
        return jnp.where(each < flag * columns, first, second)

    value = turned(probe, lax.rem(row, ROWS), lax.rem(column, LANES))
    step = LANES
    while step < columns:
        moved = jnp.concatenate([value[:, columns - step :], value[:, : columns - step]], axis=1)
        value = picked(lax.rem(lax.div(column, step), 2), moved, value)
        step *= 2
    step = ROWS
    while step < rows:
        moved = jnp.concatenate([value[rows - step :], value[: rows - step]], axis=0)
        value = picked(lax.rem(lax.div(row, step), 2), moved, value)
        step *= 2
    return picked(live, value, 0.0)


def add_terms(positions_ref, padded_ref, probes_ref, measured_ref, table_ref, grad_ref):
    planes = padded_ref.shape[0]
    slots, size, _ = measured_ref.shape

    def group(begin, width):
        terms = [[] for _ in range(width)]
        side_by_side(
            slot_stages(begin + k, positions_ref, padded_ref, probes_ref, measured_ref, table_ref, terms[k])
            for k in range(width)
        )
        for p in range(planes):
            for k, (r, c) in enumerate(itertools.product((0, size), (0, size))):
                grad_ref[p, r : r + size, c : c + size] += sum(term[p][k] for term in terms)

    @pl.loop(0, slots // PAIR)
    def _(step):
        group(step * PAIR, PAIR)

    for slot in range(slots // PAIR * PAIR, slots):
        group(slot, 1)


MESH = pl.DeviceIdType.MESH


class Around:
    def __init__(self, send_sems, recv_sems):
        self.send_sems, self.recv_sems = send_sems, recv_sems
        self.sends = self.recvs = 0
        self.here, self.device = {}, {}
        for axis in ("rows", "cols"):
            count = lax.axis_size(axis)
            me = lax.axis_index(axis)
            for d in (-2, -1, 1, 2):
                self.here[axis, d] = me + d >= 0 if d < 0 else me + d < count
                self.device[axis, d] = {axis: lax.rem(me + count + d, count)}
        count = lax.axis_size("rows")
        self.relays = count > 2 and count % 2 == 0
        odd = lax.rem(lax.axis_index("rows"), 2) == 1
        self.far = {1: odd, -1: no(odd)}
        even = lax.rem(lax.axis_index("cols"), 2) == 0
        self.quick = {1: even, -1: no(even)}

    def meet(self, meanwhile):
        barrier = pltpu.get_barrier_semaphore()
        sides = [("rows", -1), ("rows", 1), ("cols", -1), ("cols", 1)]
        if self.relays:
            sides += [("rows", -2), ("rows", 2)]
        for side in sides:

            @pl.when(self.here[side])
            def _():
                pl.semaphore_signal(barrier, inc=1, device_id=self.device[side], device_id_type=MESH)

        meanwhile()
        pl.semaphore_wait(barrier, sum(self.here[side].astype(jnp.int32) for side in sides))

    def new_recv(self):
        self.recvs += 1
        return self.recvs - 1

    def copy(self, side, source, target, recv=None):
        recv = self.new_recv() if recv is None else recv
        self.sends += 1
        return pltpu.make_async_remote_copy(
            src_ref=source,
            dst_ref=target,
            send_sem=self.send_sems.at[self.sends - 1],
            recv_sem=self.recv_sems.at[recv],
            device_id=self.device[side],
            device_id_type=MESH,
        )


class Side:
    def __init__(self, around, axis, d, source, target):
        self.here, self.back = around.here[axis, d], around.here[axis, -d]
        self.straight = around.copy((axis, d), source, target)

    def start(self):
        pl.when(self.here)(self.straight.start)

    def forward(self):
        pass

    def wait_recv(self):
        pl.when(self.back)(self.straight.wait_recv)

    def wait_left(self):
        pl.when(self.here)(self.straight.wait_send)

    def wait_forwarded(self):
        pass


class Hop:
    def __init__(self, around, d, c, source, target, relay):
        here = around.here["rows", d]
        by = both(around.far[d], around.quick[c]) if around.relays else False
        self.back = around.here["rows", -d]
        recv = around.new_recv()
        self.straight = around.copy(("rows", d), source, target, recv)
        self.near = both(here, no(by))
        self.long = both(here, by)
        self.middle = both(around.here["rows", -2 * d], by)
        self.first = around.copy(("rows", 2 * d), source, relay)
        self.second = around.copy(("rows", -d), relay, target, recv)

    def start(self):
        pl.when(self.near)(self.straight.start)
        pl.when(self.long)(self.first.start)

    def forward(self):
        @pl.when(self.middle)
        def _():
            self.first.wait_recv()
            self.second.start()

    def wait_recv(self):
        pl.when(self.back)(self.straight.wait_recv)

    def wait_left(self):
        pl.when(self.near)(self.straight.wait_send)
        pl.when(self.long)(self.first.wait_send)

    def wait_forwarded(self):
        pl.when(self.middle)(self.second.wait_send)


def both(first, second):
    return jnp.logical_and(first, second)


def no(flag):
    return jnp.logical_not(flag)


def pad(around, field_ref, out_ref, relay_ref, meanwhile, afterwards):
    m = MARGIN
    planes, high, wide = field_ref.shape
    here = around.here
    sides = (-1, 1)
    row_from = {-1: pl.ds(0, m), 1: pl.ds(high - m, m)}
    row_land = {1: pl.ds(0, m), -1: pl.ds(m + high, m)}
    half = {-1: pl.ds(0, m), 1: pl.ds(wide - m, m)}
    inner = {-1: pl.ds(m, m), 1: pl.ds(wide, m)}
    col_cuts = {-1: (pl.ds(0, m), pl.ds(m + wide, m)), 1: (pl.ds(wide - m, m), pl.ds(0, m))}
    from_cuts = {-1: pl.ds(0, m), 1: pl.ds(m + high, m)}
    rows, cols, corners = {}, {}, {}
    for d in sides:
        cut, land = col_cuts[d]
        cols[d] = Side(around, "cols", d, field_ref.at[:, :, cut], out_ref.at[:, pl.ds(m, high), land])
        for c in sides:
            source, target = field_ref.at[:, row_from[d], half[c]], out_ref.at[:, row_land[d], inner[c]]
            rows[d, c] = Hop(around, d, c, source, target, relay_ref.at[0, :, pl.ds(0, m), pl.ds(0, m)])
            corners[d, c] = around.copy(
                ("cols", c), out_ref.at[:, from_cuts[d], inner[c]], out_ref.at[:, from_cuts[d], col_cuts[c][1]]
            )

    def slow_first(work):
        for c in sides:
            pl.when(around.quick[-c])(functools.partial(work, (c, -c)))

    @slow_first
    def _(order):
        for c in order:
            for d in sides:
                rows[d, c].start()

    for d in sides:
        cols[d].start()
    for v in (-1, 1):

        @pl.when(no(here["rows", v]))
        def _():
            out_ref[:, from_cuts[v], m : m + wide] = jnp.zeros((planes, m, wide), jnp.float32)

        for d in (-1, 1):
            land = col_cuts[-d][1]

            @pl.when(no(both(here["rows", v], here["cols", d])))
            def _():
                out_ref[:, from_cuts[v], land] = jnp.zeros((planes, m, m), jnp.float32)

    for d in (-1, 1):
        land = col_cuts[-d][1]

        @pl.when(no(here["cols", d]))
        def _():
            out_ref[:, m : m + high, land] = jnp.zeros((planes, high, m), jnp.float32)

    meanwhile()
    for hop in rows.values():
        hop.forward()
    afterwards()

    def receive(far, order):
        for c in order:
            for v in (-far, far):
                rows[-v, c].wait_recv()
                pl.when(both(here["rows", v], here["cols", c]))(corners[v, c].start)

    for far in sides:
        pl.when(around.far[far])(lambda far=far: slow_first(functools.partial(receive, far)))
    for d in sides:
        cols[-d].wait_recv()
        for v in sides:
            pl.when(both(here["rows", v], here["cols", d]))(corners[v, -d].wait_recv)

    def rest():
        for copy in [*rows.values(), *cols.values()]:
            copy.wait_left()
            copy.wait_forwarded()
        for v, c in corners:
            pl.when(both(here["rows", v], here["cols", c]))(corners[v, c].wait_send)

    return rest


def step(last, around, grad_ref, padded_ref, out_ref, mid_ref, side_ref, band_ref, relay_ref, meanwhile):
    m = MARGIN
    planes, extent, _ = grad_ref.shape
    wide = extent - 2 * m
    part = extent // 2 // BLOCKS
    outside = m // part
    here = around.here
    begin = {(h, q): q * part if h < 0 else extent - (q + 1) * part for q in range(BLOCKS) for h in (-1, 1)}
    lines = {key: pl.ds(start, part) for key, start in begin.items()}
    cut = {-1: pl.ds(0, m), 1: pl.ds(extent - m, m)}
    inner = {-1: pl.ds(m, m), 1: pl.ds(wide, m)}
    half = {-1: pl.ds(0, m), 1: pl.ds(wide - m, m)}
    sent = range(outside if last else BLOCKS)
    sides, bands, edges = {}, {}, {}
    for h, q in lines:
        for d in (-1, 1):
            rows = lines[h, q]
            sides[h, q, d] = Side(around, "cols", d, grad_ref.at[:, rows, cut[d]], side_ref.at[(d + 1) // 2, :, rows])
            if not last:
                edges[h, q, d] = Side(around, "cols", d, out_ref.at[:, rows, inner[d]], out_ref.at[:, rows, cut[-d]])
            if q in sent:
                source, target = mid_ref.at[:, rows, half[d]], band_ref.at[:, lines[-h, BLOCKS - 1 - q], half[d]]
                relay = relay_ref.at[q, :, pl.ds(0, part), pl.ds(0, m)]
                bands[h, q, d] = Hop(around, h, d, source, target, relay)
    for side in sides.values():
        side.start()
    if not last:
        for d in (-1, 1):

            @pl.when(no(here["cols", d]))
            def _():
                out_ref[:, :, cut[d]] = jnp.zeros((planes, extent, m), jnp.float32)

    def gather(h, q, d):
        rows = lines[h, q]
        mid_ref[:, rows, half[d]] = grad_ref[:, rows, inner[d]]

        @pl.when(here["cols", d])
        def _():
            sides[h, q, -d].straight.wait_recv()
            mid_ref[:, rows, half[d]] += side_ref[(1 - d) // 2, :, rows]

    def finish(h, q, d):
        rows = lines[h, q]
        place = (slice(None), pl.ds(rows.start - m, part), half[d]) if last else (slice(None), rows, inner[d])

        @pl.when(here["rows", h])
        def _():
            bands[-h, BLOCKS - 1 - q, d].straight.wait_recv()
            total = mid_ref[:, rows, half[d]] + band_ref[:, rows, half[d]]
            out_ref[place] = padded_ref[:, rows, inner[d]] - step_rate * total

        @pl.when(no(here["rows", h]))
        def _():
            if q < outside:
                out_ref[place] = jnp.zeros((planes, part, m), jnp.float32)
            else:
                out_ref[place] = padded_ref[:, rows, inner[d]] - step_rate * mid_ref[:, rows, half[d]]

        if not last:
            edges[h, q, d].start()

    def in_turn(far, quick):
        near, straight = [(-far, q, quick) for q in sent], []
        relayed = [(far, q, quick) for q in sent]
        for q in sent:
            straight += [(-far, q, -quick), (far, q, -quick)]
        return near, straight, relayed

    def begin_all(far, quick):
        near, straight, relayed = in_turn(far, quick)
        for h, q, d in near[:1] + relayed + straight + near[1:]:
            gather(h, q, d)
            bands[h, q, d].start()
        for h, q, d in sides:
            if q not in sent:
                gather(h, q, d)

    def finish_all(far, quick):
        near, straight, relayed = in_turn(far, quick)
        for h, q, d in near[:1] + straight + near[1:] + relayed:
            finish(h, BLOCKS - 1 - q, d)

    def by_place(work):
        for far in (-1, 1):
            for quick in (-1, 1):
                pl.when(both(around.far[far], around.quick[quick]))(functools.partial(work, far, quick))

    by_place(begin_all)
    for band in bands.values():
        band.forward()
    meanwhile()
    by_place(finish_all)
    for edge in edges.values():
        edge.wait_recv()
    def rest():
        for copy in [*bands.values(), *edges.values(), *sides.values()]:
            copy.wait_left()
            copy.wait_forwarded()

    return rest


def whole_kernel(
    positions_ref,
    counts_ref,
    field_ref,
    intensity_ref,
    probe_from,
    table_from,
    out_ref,
    *refs,
):
    padded_refs, refs = refs[:ITERS], refs[ITERS:]
    work(
        positions_ref, counts_ref, field_ref, intensity_ref, probe_from, table_from, out_ref, padded_refs, *refs
    )


def work(
    positions_ref,
    counts_ref,
    field_ref,
    intensity_ref,
    probe_from,
    table_from,
    out_ref,
    padded_refs,
    grad_ref,
    measured_ref,
    probes_ref,
    raw_ref,
    probe_ref,
    table_ref,
    mid_ref,
    side_ref,
    band_ref,
    relay_ref,
    send_sems,
    recv_sems,
    local_sems,
):
    m = MARGIN
    planes, high, wide = field_ref.shape
    slots, size, _ = measured_ref.shape
    parts = size // LANES
    own = pltpu.make_async_copy(
        field_ref, padded_refs[0].at[:, pl.ds(m, high), pl.ds(m, wide)], local_sems.at[slots * parts]
    )
    fetches = [
        pltpu.make_async_copy(
            intensity_ref.at[0, 0, k, :, pl.ds(c * LANES, LANES)], raw_ref.at[k, c], local_sems.at[k * parts + c]
        )
        for k in range(slots)
        for c in range(parts)
    ]
    held = [
        pltpu.make_async_copy(source, target, local_sems.at[slots * parts + 1 + k])
        for k, (source, target) in enumerate([(probe_from, probe_ref), (table_from, table_ref)])
    ]
    around = Around(send_sems, recv_sems)

    def fetch_all():
        for copy in [*fetches, own, *held]:
            copy.start()

    around.meet(fetch_all)

    def meanwhile():
        grad_ref[...] = jnp.zeros_like(grad_ref)
        order = order_columns(size)
        for k in range(slots):
            for c in range(parts):
                fetches[k * parts + c].wait()
            put_in_order(raw_ref.at[k], measured_ref.at[k], order)

    def afterwards():
        for copy in [own, *held]:
            copy.wait()

        @pl.loop(0, slots)
        def _(slot):
            live = counts_ref[0, 0] - slot
            for p in range(planes):
                probes_ref[slot, p] = roll_probe(live, positions_ref[0, slot], positions_ref[1, slot], probe_ref[p])

    rest = pad(around, field_ref, padded_refs[0], relay_ref.at[0], meanwhile, afterwards)
    for k in range(ITERS):
        last = k == ITERS - 1
        add_terms(positions_ref, padded_refs[k], probes_ref, measured_ref, table_ref, grad_ref.at[k])
        target = out_ref if last else padded_refs[k + 1]
        scratch = [ref.at[k] for ref in (mid_ref, side_ref, band_ref)]
        rest = step(
            last, around, grad_ref.at[k], padded_refs[k], target, *scratch, relay_ref.at[k + 1], meanwhile=rest
        )
    rest()


def on_device(object_field, probe, positions, counts, intensity):
    planes, high, wide = object_field.shape
    slots, size, _ = intensity.shape[2:]
    table = jnp.asarray(tables(size))
    tall, broad = high + 2 * MARGIN, wide + 2 * MARGIN
    assert tall == broad == 2 * size and wide == 2 * MARGIN
    copies = 64 * (ITERS + 1)
    floats = [
        *[(planes, tall, broad)] * ITERS,
        (ITERS, planes, tall, broad),
        (slots, size, size),
        (slots, planes, size, size),
    ]
    blocks = [
        (ITERS, planes, tall, wide),
        (ITERS, 2, planes, tall, MARGIN),
        (ITERS, planes, tall, wide),
        (ITERS + 1, BLOCKS, planes, MARGIN, MARGIN),
    ]
    held = [pltpu.with_memory_space_constraint(array, pltpu.HBM) for array in (object_field, intensity, probe, table)]
    return pl.pallas_call(
        whole_kernel,
        out_shape=jax.ShapeDtypeStruct(object_field.shape, jnp.float32),
        in_specs=[pl.BlockSpec(memory_space=pltpu.SMEM)] * 2 + [pl.BlockSpec(memory_space=pltpu.HBM)] * len(held),
        out_specs=pl.BlockSpec(memory_space=pltpu.VMEM),
        scratch_shapes=[pltpu.VMEM(shape, jnp.float32) for shape in floats]
        + [
            pltpu.VMEM((slots, size // LANES, size, LANES), jnp.int32),
            pltpu.VMEM(probe.shape, jnp.float32),
            pltpu.VMEM(table.shape, jnp.bfloat16),
        ]
        + [pltpu.VMEM(shape, jnp.float32) for shape in blocks]
        + [
            pltpu.SemaphoreType.DMA((copies,)),
            pltpu.SemaphoreType.DMA((copies,)),
            pltpu.SemaphoreType.DMA((slots * (size // LANES) + 3,)),
        ],
        compiler_params=pltpu.CompilerParams(
            collective_id=0, has_side_effects=True, vmem_limit_bytes=48 * 1024 * 1024
        ),
        name="whole",
    )(positions[0, 0].T, counts, *held)


def solution(mesh):
    placed = (
        P(None, "rows", "cols"),
        P(),
        P("rows", "cols", None, None),
        P("rows", "cols"),
        P("rows", "cols", None, None, None),
    )
    return jax.shard_map(
        on_device, mesh=mesh, in_specs=placed, out_specs=P(None, "rows", "cols"), check_vma=False
    )
```

```python
import functools
import itertools

import jax
import jax.numpy as jnp
import numpy as np
from jax import lax
from jax.experimental import pallas as pl
from jax.experimental.pallas import tpu as pltpu
from jax.sharding import PartitionSpec as P

MARGIN = 128
ITERS = 2
LANES = 128
ROWS = 8
PAIR = 2
BLOCKS = 4


step_rate = 0.02
photon_unit = 0.001


def tables(length):
    half = length // 2
    k = np.arange(half)[:, None]
    n = np.arange(half)[None, :]
    found = []
    for odd in (0, 1):
        angle = ((2 * k + odd) * n % length) * (2.0 * np.pi / length)
        c = np.cos(angle) / np.sqrt(length)
        s = np.sin(angle) / np.sqrt(length)
        full = np.block([[c, s], [-s, c]])
        found += [full, full.T]
    full = np.stack(found).astype(np.float32)
    high = full.astype(jnp.bfloat16)
    low = (full - high.astype(np.float32)).astype(jnp.bfloat16)
    return np.stack([high, low])


def dot(left, right):
    return lax.dot_general(left, right, (((1,), (0,)), ((), ())), preferred_element_type=jnp.float32)


def parted(value):
    high = value.astype(jnp.bfloat16)
    return high, (value - high.astype(jnp.float32)).astype(jnp.bfloat16)


def order_columns(length):
    half = length // 2
    here = lax.broadcasted_iota(jnp.int32, (length, length), 0)
    there = lax.broadcasted_iota(jnp.int32, (length, length), 1)
    wanted = jnp.where(there < half, 2 * there, 2 * there - length + 1)
    return jnp.where(here == wanted, 1.0, 0.0).astype(jnp.bfloat16)


def put_in_order(raw_ref, measured_ref, order):
    parts, size, _ = raw_ref.shape
    given = jnp.concatenate(
        [
            jnp.concatenate([raw_ref[c, pl.ds(odd, size // 2, stride=2)] for c in range(parts)], axis=1)
            for odd in (0, 1)
        ],
        axis=0,
    )

    def placed(value):
        return dot(value.astype(jnp.float32).astype(jnp.bfloat16), order)

    measured_ref[...] = (placed(given >> 4) * 16.0 + placed(given & 15)) * photon_unit


def from_left(table, which, value):
    high, low = value
    table = jnp.concatenate([table[0, which], table[1, which], table[0, which]], axis=1)
    return dot(table, jnp.concatenate([high, high, low], axis=0))


def from_right(table, which, value):
    high, low = value
    table = jnp.concatenate([table[0, which], table[1, which], table[0, which]], axis=0)
    return dot(jnp.concatenate([high, high, low], axis=1), table)


def turned(value, drop, shift):
    rows, columns = value.shape
    groups = pltpu.roll(value.reshape(rows // ROWS, ROWS, columns), drop, 1)
    before = jnp.concatenate([groups[-1:], groups[:-1]], axis=0)
    within = lax.broadcasted_iota(jnp.int32, (1, ROWS, columns), 1) >= drop
    value = jnp.where(within, groups, before).reshape(rows, columns)
    parts = [pltpu.roll(value[:, c : c + LANES], shift, 1) for c in range(0, columns, LANES)]
    within = lax.broadcasted_iota(jnp.int32, (rows, LANES), 1) >= shift
    return jnp.concatenate([jnp.where(within, a, b) for a, b in zip(parts, parts[-1:] + parts[:-1])], axis=1)


def slot_stages(slot, positions_ref, padded_ref, probes_ref, measured_ref, table_ref, terms):
    size = probes_ref.shape[2]
    half = size // 2
    below = lax.broadcasted_iota(jnp.int32, (size, size), 0) >= positions_ref[0, slot]
    beside = lax.broadcasted_iota(jnp.int32, (size, size), 1) >= positions_ref[1, slot]

    def folded(p):
        upper = jnp.where(beside, padded_ref[p, :size, :size], padded_ref[p, :size, size:])
        lower = jnp.where(beside, padded_ref[p, size:, :size], padded_ref[p, size:, size:])
        return jnp.where(below, upper, lower)

    probe_r = probes_ref[slot, 0]
    probe_i = probes_ref[slot, 1]
    patch_r, patch_i = folded(0), folded(1)
    exit_r = probe_r * patch_r - probe_i * patch_i
    exit_i = probe_r * patch_i + probe_i * patch_r
    upper = jnp.concatenate([exit_r[:half], exit_i[:half]], axis=0)
    lower = jnp.concatenate([exit_r[half:], exit_i[half:]], axis=0)
    even, odd = parted(upper + lower), parted(upper - lower)
    yield
    even, odd = from_left(table_ref, 0, even), from_left(table_ref, 2, odd)
    yield
    half_r = jnp.concatenate([even[:half], odd[:half]], axis=0)
    half_i = jnp.concatenate([even[half:], odd[half:]], axis=0)
    left = jnp.concatenate([half_r[:, :half], half_i[:, :half]], axis=1)
    right = jnp.concatenate([half_r[:, half:], half_i[:, half:]], axis=1)
    values = [parted(left + right), parted(left - right)]
    yield
    specs = [from_right(table_ref, 2 * odd + 1, value) for odd, value in enumerate(values)]
    yield
    values = []
    for odd, spec in enumerate(specs):
        spec_r, spec_i = spec[:, :half], spec[:, half:]
        misfit = spec_r * spec_r + spec_i * spec_i - measured_ref[slot, :, odd * half : (odd + 1) * half]
        values.append(parted(jnp.concatenate([misfit * spec_r, misfit * spec_i], axis=1)))
    yield
    backs = [from_right(table_ref, 2 * odd, value) for odd, value in enumerate(values)]
    yield
    left = backs[0] + backs[1]
    right = backs[0] - backs[1]
    half_r = jnp.concatenate([left[:, :half], right[:, :half]], axis=1)
    half_i = jnp.concatenate([left[:, half:], right[:, half:]], axis=1)
    even = parted(jnp.concatenate([half_r[:half], half_i[:half]], axis=0))
    odd = parted(jnp.concatenate([half_r[half:], half_i[half:]], axis=0))
    yield
    even, odd = from_left(table_ref, 1, even), from_left(table_ref, 3, odd)
    yield
    upper = even + odd
    lower = even - odd
    back_r = jnp.concatenate([upper[:half], lower[:half]], axis=0)
    back_i = jnp.concatenate([upper[half:], lower[half:]], axis=0)
    term_r = probe_r * back_r + probe_i * back_i
    term_i = probe_r * back_i - probe_i * back_r
    for term in (term_r, term_i):
        upper, lower = jnp.where(below, term, 0.0), jnp.where(below, 0.0, term)
        terms.append([jnp.where(beside, t, 0.0) if left else jnp.where(beside, 0.0, t) for t in (upper, lower) for left in (1, 0)])


def side_by_side(works):
    works = list(works)
    while works:
        works = [work for work in works if next(work, works) is not works]


def roll_probe(live, row, column, probe):
    rows, columns = probe.shape
    each = lax.broadcasted_iota(jnp.int32, probe.shape, 1)

    def picked(flag, first, second):
        return jnp.where(each < flag * columns, first, second)

    value = turned(probe, lax.rem(row, ROWS), lax.rem(column, LANES))
    step = LANES
    while step < columns:
        moved = jnp.concatenate([value[:, columns - step :], value[:, : columns - step]], axis=1)
        value = picked(lax.rem(lax.div(column, step), 2), moved, value)
        step *= 2
    step = ROWS
    while step < rows:
        moved = jnp.concatenate([value[rows - step :], value[: rows - step]], axis=0)
        value = picked(lax.rem(lax.div(row, step), 2), moved, value)
        step *= 2
    return picked(live, value, 0.0)


def add_terms(positions_ref, padded_ref, probes_ref, measured_ref, table_ref, grad_ref):
    planes = padded_ref.shape[0]
    slots, size, _ = measured_ref.shape

    def group(begin, width):
        terms = [[] for _ in range(width)]
        side_by_side(
            slot_stages(begin + k, positions_ref, padded_ref, probes_ref, measured_ref, table_ref, terms[k])
            for k in range(width)
        )
        for p in range(planes):
            for k, (r, c) in enumerate(itertools.product((0, size), (0, size))):
                grad_ref[p, r : r + size, c : c + size] += sum(term[p][k] for term in terms)

    @pl.loop(0, slots // PAIR)
    def _(step):
        group(step * PAIR, PAIR)

    for slot in range(slots // PAIR * PAIR, slots):
        group(slot, 1)


MESH = pl.DeviceIdType.MESH


class Around:
    def __init__(self, send_sems, recv_sems):
        self.send_sems, self.recv_sems = send_sems, recv_sems
        self.sends = self.recvs = 0
        self.here, self.device = {}, {}
        for axis in ("rows", "cols"):
            count = lax.axis_size(axis)
            me = lax.axis_index(axis)
            for d in (-2, -1, 1, 2):
                self.here[axis, d] = me + d >= 0 if d < 0 else me + d < count
                self.device[axis, d] = {axis: lax.rem(me + count + d, count)}
        count = lax.axis_size("rows")
        self.relays = count > 2 and count % 2 == 0
        odd = lax.rem(lax.axis_index("rows"), 2) == 1
        self.far = {1: odd, -1: no(odd)}
        even = lax.rem(lax.axis_index("cols"), 2) == 0
        self.quick = {1: even, -1: no(even)}

    def meet(self, meanwhile):
        barrier = pltpu.get_barrier_semaphore()
        sides = [("rows", -1), ("rows", 1), ("cols", -1), ("cols", 1)]
        if self.relays:
            sides += [("rows", -2), ("rows", 2)]
        for side in sides:

            @pl.when(self.here[side])
            def _():
                pl.semaphore_signal(barrier, inc=1, device_id=self.device[side], device_id_type=MESH)

        meanwhile()
        pl.semaphore_wait(barrier, sum(self.here[side].astype(jnp.int32) for side in sides))

    def new_recv(self):
        self.recvs += 1
        return self.recvs - 1

    def copy(self, side, source, target, recv=None):
        recv = self.new_recv() if recv is None else recv
        self.sends += 1
        return pltpu.make_async_remote_copy(
            src_ref=source,
            dst_ref=target,
            send_sem=self.send_sems.at[self.sends - 1],
            recv_sem=self.recv_sems.at[recv],
            device_id=self.device[side],
            device_id_type=MESH,
        )


class Side:
    def __init__(self, around, axis, d, source, target):
        self.here, self.back = around.here[axis, d], around.here[axis, -d]
        self.straight = around.copy((axis, d), source, target)

    def start(self):
        pl.when(self.here)(self.straight.start)

    def forward(self):
        pass

    def wait_recv(self):
        pl.when(self.back)(self.straight.wait_recv)

    def wait_left(self):
        pl.when(self.here)(self.straight.wait_send)

    def wait_forwarded(self):
        pass


class Hop:
    def __init__(self, around, d, c, source, target, relay):
        here = around.here["rows", d]
        by = both(around.far[d], around.quick[c]) if around.relays else False
        self.back = around.here["rows", -d]
        recv = around.new_recv()
        self.straight = around.copy(("rows", d), source, target, recv)
        self.near = both(here, no(by))
        self.long = both(here, by)
        self.middle = both(around.here["rows", -2 * d], by)
        self.first = around.copy(("rows", 2 * d), source, relay)
        self.second = around.copy(("rows", -d), relay, target, recv)

    def start(self):
        pl.when(self.near)(self.straight.start)
        pl.when(self.long)(self.first.start)

    def forward(self):
        @pl.when(self.middle)
        def _():
            self.first.wait_recv()
            self.second.start()

    def wait_recv(self):
        pl.when(self.back)(self.straight.wait_recv)

    def wait_left(self):
        pl.when(self.near)(self.straight.wait_send)
        pl.when(self.long)(self.first.wait_send)

    def wait_forwarded(self):
        pl.when(self.middle)(self.second.wait_send)


def both(first, second):
    return jnp.logical_and(first, second)


def no(flag):
    return jnp.logical_not(flag)


def pad(around, field_ref, out_ref, relay_ref, meanwhile, afterwards):
    m = MARGIN
    planes, high, wide = field_ref.shape
    here = around.here
    sides = (-1, 1)
    row_from = {-1: pl.ds(0, m), 1: pl.ds(high - m, m)}
    row_land = {1: pl.ds(0, m), -1: pl.ds(m + high, m)}
    half = {-1: pl.ds(0, m), 1: pl.ds(wide - m, m)}
    inner = {-1: pl.ds(m, m), 1: pl.ds(wide, m)}
    col_cuts = {-1: (pl.ds(0, m), pl.ds(m + wide, m)), 1: (pl.ds(wide - m, m), pl.ds(0, m))}
    from_cuts = {-1: pl.ds(0, m), 1: pl.ds(m + high, m)}
    rows, cols, corners = {}, {}, {}
    for d in sides:
        cut, land = col_cuts[d]
        cols[d] = Side(around, "cols", d, field_ref.at[:, :, cut], out_ref.at[:, pl.ds(m, high), land])
        for c in sides:
            source, target = field_ref.at[:, row_from[d], half[c]], out_ref.at[:, row_land[d], inner[c]]
            rows[d, c] = Hop(around, d, c, source, target, relay_ref.at[0, :, pl.ds(0, m), pl.ds(0, m)])
            corners[d, c] = around.copy(
                ("cols", c), out_ref.at[:, from_cuts[d], inner[c]], out_ref.at[:, from_cuts[d], col_cuts[c][1]]
            )

    def slow_first(work):
        for c in sides:
            pl.when(around.quick[-c])(functools.partial(work, (c, -c)))

    @slow_first
    def _(order):
        for c in order:
            for d in sides:
                rows[d, c].start()

    for d in sides:
        cols[d].start()
    for v in (-1, 1):

        @pl.when(no(here["rows", v]))
        def _():
            out_ref[:, from_cuts[v], m : m + wide] = jnp.zeros((planes, m, wide), jnp.float32)

        for d in (-1, 1):
            land = col_cuts[-d][1]

            @pl.when(no(both(here["rows", v], here["cols", d])))
            def _():
                out_ref[:, from_cuts[v], land] = jnp.zeros((planes, m, m), jnp.float32)

    for d in (-1, 1):
        land = col_cuts[-d][1]

        @pl.when(no(here["cols", d]))
        def _():
            out_ref[:, m : m + high, land] = jnp.zeros((planes, high, m), jnp.float32)

    meanwhile()
    for hop in rows.values():
        hop.forward()
    afterwards()

    def receive(far, order):
        for c in order:
            for v in (-far, far):
                rows[-v, c].wait_recv()
                pl.when(both(here["rows", v], here["cols", c]))(corners[v, c].start)

    for far in sides:
        pl.when(around.far[far])(lambda far=far: slow_first(functools.partial(receive, far)))
    for d in sides:
        cols[-d].wait_recv()
        for v in sides:
            pl.when(both(here["rows", v], here["cols", d]))(corners[v, -d].wait_recv)

    def rest():
        for copy in [*rows.values(), *cols.values()]:
            copy.wait_left()
            copy.wait_forwarded()
        for v, c in corners:
            pl.when(both(here["rows", v], here["cols", c]))(corners[v, c].wait_send)

    return rest


def step(last, around, grad_ref, padded_ref, out_ref, mid_ref, side_ref, band_ref, relay_ref, meanwhile):
    m = MARGIN
    planes, extent, _ = grad_ref.shape
    wide = extent - 2 * m
    part = extent // 2 // BLOCKS
    outside = m // part
    here = around.here
    begin = {(h, q): q * part if h < 0 else extent - (q + 1) * part for q in range(BLOCKS) for h in (-1, 1)}
    lines = {key: pl.ds(start, part) for key, start in begin.items()}
    cut = {-1: pl.ds(0, m), 1: pl.ds(extent - m, m)}
    inner = {-1: pl.ds(m, m), 1: pl.ds(wide, m)}
    half = {-1: pl.ds(0, m), 1: pl.ds(wide - m, m)}
    sent = range(outside if last else BLOCKS)
    sides, bands, edges = {}, {}, {}
    for h, q in lines:
        for d in (-1, 1):
            rows = lines[h, q]
            sides[h, q, d] = Side(around, "cols", d, grad_ref.at[:, rows, cut[d]], side_ref.at[(d + 1) // 2, :, rows])
            if not last:
                edges[h, q, d] = Side(around, "cols", d, out_ref.at[:, rows, inner[d]], out_ref.at[:, rows, cut[-d]])
            if q in sent:
                source, target = mid_ref.at[:, rows, half[d]], band_ref.at[:, lines[-h, BLOCKS - 1 - q], half[d]]
                relay = relay_ref.at[q, :, pl.ds(0, part), pl.ds(0, m)]
                bands[h, q, d] = Hop(around, h, d, source, target, relay)
    for side in sides.values():
        side.start()
    if not last:
        for d in (-1, 1):

            @pl.when(no(here["cols", d]))
            def _():
                out_ref[:, :, cut[d]] = jnp.zeros((planes, extent, m), jnp.float32)

    def gather(h, q, d):
        rows = lines[h, q]
        mid_ref[:, rows, half[d]] = grad_ref[:, rows, inner[d]]

        @pl.when(here["cols", d])
        def _():
            sides[h, q, -d].straight.wait_recv()
            mid_ref[:, rows, half[d]] += side_ref[(1 - d) // 2, :, rows]

    def finish(h, q, d):
        rows = lines[h, q]
        place = (slice(None), pl.ds(rows.start - m, part), half[d]) if last else (slice(None), rows, inner[d])

        @pl.when(here["rows", h])
        def _():
            bands[-h, BLOCKS - 1 - q, d].straight.wait_recv()
            total = mid_ref[:, rows, half[d]] + band_ref[:, rows, half[d]]
            out_ref[place] = padded_ref[:, rows, inner[d]] - step_rate * total

        @pl.when(no(here["rows", h]))
        def _():
            if q < outside:
                out_ref[place] = jnp.zeros((planes, part, m), jnp.float32)
            else:
                out_ref[place] = padded_ref[:, rows, inner[d]] - step_rate * mid_ref[:, rows, half[d]]

        if not last:
            edges[h, q, d].start()

    def in_turn(far, quick):
        near, straight = [(-far, q, quick) for q in sent], []
        relayed = [(far, q, quick) for q in sent]
        for q in sent:
            straight += [(-far, q, -quick), (far, q, -quick)]
        return near, straight, relayed

    def begin_all(far, quick):
        near, straight, relayed = in_turn(far, quick)
        for h, q, d in near[:1] + relayed + straight + near[1:]:
            gather(h, q, d)
            bands[h, q, d].start()
        for h, q, d in sides:
            if q not in sent:
                gather(h, q, d)

    def finish_all(far, quick):
        near, straight, relayed = in_turn(far, quick)
        for h, q, d in near[:1] + straight + near[1:] + relayed:
            finish(h, BLOCKS - 1 - q, d)

    def by_place(work):
        for far in (-1, 1):
            for quick in (-1, 1):
                pl.when(both(around.far[far], around.quick[quick]))(functools.partial(work, far, quick))

    by_place(begin_all)
    for band in bands.values():
        band.forward()
    meanwhile()
    by_place(finish_all)
    for edge in edges.values():
        edge.wait_recv()
    def rest():
        for copy in [*bands.values(), *edges.values(), *sides.values()]:
            copy.wait_left()
            copy.wait_forwarded()

    return rest


def whole_kernel(
    positions_ref,
    counts_ref,
    field_ref,
    intensity_ref,
    probe_from,
    table_from,
    out_ref,
    *refs,
):
    padded_refs, refs = refs[:ITERS], refs[ITERS:]
    work(
        positions_ref, counts_ref, field_ref, intensity_ref, probe_from, table_from, out_ref, padded_refs, *refs
    )


def work(
    positions_ref,
    counts_ref,
    field_ref,
    intensity_ref,
    probe_from,
    table_from,
    out_ref,
    padded_refs,
    grad_ref,
    measured_ref,
    probes_ref,
    raw_ref,
    probe_ref,
    table_ref,
    mid_ref,
    side_ref,
    band_ref,
    relay_ref,
    send_sems,
    recv_sems,
    local_sems,
):
    m = MARGIN
    planes, high, wide = field_ref.shape
    slots, size, _ = measured_ref.shape
    parts = size // LANES
    own = pltpu.make_async_copy(
        field_ref, padded_refs[0].at[:, pl.ds(m, high), pl.ds(m, wide)], local_sems.at[slots * parts]
    )
    fetches = [
        pltpu.make_async_copy(
            intensity_ref.at[0, 0, k, :, pl.ds(c * LANES, LANES)], raw_ref.at[k, c], local_sems.at[k * parts + c]
        )
        for k in range(slots)
        for c in range(parts)
    ]
    held = [
        pltpu.make_async_copy(source, target, local_sems.at[slots * parts + 1 + k])
        for k, (source, target) in enumerate([(probe_from, probe_ref), (table_from, table_ref)])
    ]
    around = Around(send_sems, recv_sems)

    def fetch_all():
        for copy in [*fetches, own, *held]:
            copy.start()

    around.meet(fetch_all)

    def meanwhile():
        grad_ref[...] = jnp.zeros_like(grad_ref)
        order = order_columns(size)
        for k in range(slots):
            for c in range(parts):
                fetches[k * parts + c].wait()
            put_in_order(raw_ref.at[k], measured_ref.at[k], order)

    def afterwards():
        for copy in [own, *held]:
            copy.wait()

        @pl.loop(0, slots)
        def _(slot):
            live = counts_ref[0, 0] - slot
            for p in range(planes):
                probes_ref[slot, p] = roll_probe(live, positions_ref[0, slot], positions_ref[1, slot], probe_ref[p])

    rest = pad(around, field_ref, padded_refs[0], relay_ref.at[0], meanwhile, afterwards)
    for k in range(ITERS):
        last = k == ITERS - 1
        add_terms(positions_ref, padded_refs[k], probes_ref, measured_ref, table_ref, grad_ref.at[k])
        target = out_ref if last else padded_refs[k + 1]
        scratch = [ref.at[k] for ref in (mid_ref, side_ref, band_ref)]
        rest = step(
            last, around, grad_ref.at[k], padded_refs[k], target, *scratch, relay_ref.at[k + 1], meanwhile=rest
        )
    rest()


def on_device(object_field, probe, positions, counts, intensity):
    planes, high, wide = object_field.shape
    slots, size, _ = intensity.shape[2:]
    table = jnp.asarray(tables(size))
    tall, broad = high + 2 * MARGIN, wide + 2 * MARGIN
    assert tall == broad == 2 * size and wide == 2 * MARGIN
    copies = 64 * (ITERS + 1)
    floats = [
        *[(planes, tall, broad)] * ITERS,
        (ITERS, planes, tall, broad),
        (slots, size, size),
        (slots, planes, size, size),
    ]
    blocks = [
        (ITERS, planes, tall, wide),
        (ITERS, 2, planes, tall, MARGIN),
        (ITERS, planes, tall, wide),
        (ITERS + 1, BLOCKS, planes, MARGIN, MARGIN),
    ]
    held = [pltpu.with_memory_space_constraint(array, pltpu.HBM) for array in (object_field, intensity, probe, table)]
    return pl.pallas_call(
        whole_kernel,
        out_shape=jax.ShapeDtypeStruct(object_field.shape, jnp.float32),
        in_specs=[pl.BlockSpec(memory_space=pltpu.SMEM)] * 2 + [pl.BlockSpec(memory_space=pltpu.HBM)] * len(held),
        out_specs=pl.BlockSpec(memory_space=pltpu.VMEM),
        scratch_shapes=[pltpu.VMEM(shape, jnp.float32) for shape in floats]
        + [
            pltpu.VMEM((slots, size // LANES, size, LANES), jnp.int32),
            pltpu.VMEM(probe.shape, jnp.float32),
            pltpu.VMEM(table.shape, jnp.bfloat16),
        ]
        + [pltpu.VMEM(shape, jnp.float32) for shape in blocks]
        + [
            pltpu.SemaphoreType.DMA((copies,)),
            pltpu.SemaphoreType.DMA((copies,)),
            pltpu.SemaphoreType.DMA((slots * (size // LANES) + 3,)),
        ],
        compiler_params=pltpu.CompilerParams(
            collective_id=0, has_side_effects=True, vmem_limit_bytes=48 * 1024 * 1024
        ),
        name="whole",
    )(positions[0, 0].T, counts, *held)


def solution(mesh):
    placed = (
        P(None, "rows", "cols"),
        P(),
        P("rows", "cols", None, None),
        P("rows", "cols"),
        P("rows", "cols", None, None, None),
    )
    return jax.shard_map(
        on_device, mesh=mesh, in_specs=placed, out_specs=P(None, "rows", "cols"), check_vma=False
    )
```
